32 devices in a mesh: groups: 2 (over x), grid: 4 (over y, core), orb: 4 (over z).
Axes of the slice: x: 2, y: 2, z: 4, core: 2. Of those that a mesh axis runs over, the one named last changes fastest.
Arguments:
- orbitals: float32 [32, 2, 128, 128, 128], P(('groups', 'orb'), None, 'grid'), parts along dimension 0, may hold values from -6 to 6
- v_local: float32 [256, 128, 128], P(('groups', 'grid')), parts along dimension 0, may hold values from -24 to 24
- occupations: float32 [32], P('groups'), parts along dimension 0, may hold values from 0.05 to 0.5
Outputs:
- orbitals_next: float32 [32, 2, 128, 128, 128], P(('groups', 'orb'), None, 'grid'), parts along dimension 0
The draws below stay inside these ranges and needn't reach their ends.
There are 2 independent parts, one for each index of `groups`. The reference program is written for one: setup_inputs(seed, part) draws one part's arguments, and reference() takes and returns one part's arrays. A program takes and returns all parts, laid end to end along the dimension named above; each array names one. Nothing has to cross between parts.
All inputs are finite; a program needn't handle non-finite values.
Results may differ from the reference program's by a relative error of at most 0.00035.
Values sent between devices are 32-bit elements; how exact they have to be, the bound alone decides.
A program may use at most 128 MiB of HBM per device.

```python
import math
import jax
import jax.numpy as jnp
from jax import lax

NX = 128
NY = 128
NZ = 128
ORB = 16


def block_levels(rng, dims, split, low, high):
    def one(dim, blocks):
        steps = jax.random.uniform(jax.random.fold_in(jax.random.fold_in(rng, 6), dim), (blocks,), jnp.float32, low / len(split), high / len(split))
        return jnp.repeat(jnp.exp(steps), dims[dim] // blocks).reshape((-1,) + (1,) * (len(dims) - dim - 1))

    factor_of = one(*split[0])
    for cut in split[1:]:
        factor_of = factor_of * one(*cut)
    return factor_of


def bell_draw(rng, shape, spread, reach, pieces=(), dtype=jnp.bfloat16):
    array = jax.random.normal(rng, shape, jnp.float32) * spread
    if len(pieces) > 0:
        array = block_levels(rng, shape, pieces, -0.22, 0.18) * array
    return jnp.clip(array, min=-reach, max=reach).astype(dtype)


def setup_inputs(seed: int = 0, part: int = 0) -> dict:
    splits = jax.random.split(jax.random.key(seed), 4)
    own_keys = jax.random.split(jax.random.fold_in(splits[3], part), 4)
    return {
        "orbitals": bell_draw(own_keys[0], (ORB, 2, NX, NY, NZ), 1.0, 6.0, ((0, 4), (2, 4)), jnp.float32),
        "v_local": bell_draw(own_keys[1], (NX, NY, NZ), 4.0, 24.0, ((0, 4),), jnp.float32),
        "occupations": jnp.clip(jnp.exp(jax.random.uniform(own_keys[2], (ORB,), jnp.float32, math.log(0.05), math.log(0.5))), 0.05, 0.5),
    }


TIME_STEP = 0.05
KINETIC_RATE = 0.1
HARTREE_SCALE = math.pi


def wave_squared(length):
    wavenumber = jnp.fft.fftfreq(length).astype(jnp.float32) * (2.0 * math.pi)
    return wavenumber * wavenumber


def reference(orbitals, v_local, occupations):
    waves = wave_squared(NX)[:, None, None] + wave_squared(NY)[None, :, None] + wave_squared(NZ)[None, None, :]
    kinetic_turn = -KINETIC_RATE * waves
    propagator = lax.complex(jnp.cos(kinetic_turn), jnp.sin(kinetic_turn))
    spectrum = jnp.fft.fftn(lax.complex(orbitals[:, 0], orbitals[:, 1]), axes=(1, 2, 3))
    evolved = jnp.fft.ifftn(spectrum * propagator[None], axes=(1, 2, 3))
    evolved_re = jnp.real(evolved)
    evolved_im = jnp.imag(evolved)
    density = jnp.sum(occupations[:, None, None, None] * (evolved_re * evolved_re + evolved_im * evolved_im), axis=0)
    anchor = waves <= 0.0
    kernel = jnp.where(anchor, 0.0, HARTREE_SCALE / jnp.where(anchor, 1.0, waves))
    hartree = jnp.real(jnp.fft.ifftn(jnp.fft.fftn(density) * kernel))
    phase_angle = TIME_STEP * (v_local + hartree)
    cosine = jnp.cos(phase_angle)[None]
    sine = jnp.sin(phase_angle)[None]
    out_re = evolved_re * cosine + evolved_im * sine
    out_im = evolved_im * cosine - evolved_re * sine
    return jnp.stack([out_re, out_im], 1).astype(jnp.float32)
```

```python
from functools import partial
import math

import jax
import jax.numpy as jnp
import ml_dtypes
import numpy as np
from jax import lax
from jax.experimental import pallas as pl
from jax.experimental.pallas import tpu as pltpu
from jax.sharding import PartitionSpec as P

TIME_STEP = 0.05
KINETIC_RATE = 0.1
HARTREE_SCALE = math.pi
HIGHEST = lax.Precision.HIGHEST
VMEM_LIMIT = 50 * 1024 * 1024


def wave_squared(length):
    ids = np.arange(length)
    signed = np.where(ids < (length + 1) // 2, ids, ids - length)
    return (2.0 * np.pi * signed / length) ** 2


def fourier(length, sign):
    ids = np.arange(length)
    return np.exp(sign * 2j * np.pi * ((ids[:, None] * ids[None, :]) % length) / length)


def kinetic_matrix(length):
    phase = np.exp(-1j * KINETIC_RATE * wave_squared(length))
    return (fourier(length, 1) / length * phase[None, :]) @ fourier(length, -1)


def left_block(matrix):
    return np.block([[matrix.real, -matrix.imag], [matrix.imag, matrix.real]])


def right_block(matrix):
    return np.block([[matrix.real, matrix.imag], [-matrix.imag, matrix.real]])


def split_const(table):
    table = np.asarray(table, np.float32)
    high = table.astype(ml_dtypes.bfloat16)
    low = (table - high.astype(np.float32)).astype(ml_dtypes.bfloat16)
    return np.stack([high, low])


def split(values):
    high = values.astype(jnp.bfloat16)
    low = (values - high.astype(jnp.float32)).astype(jnp.bfloat16)
    return high, low


def dot(left, right):
    return jnp.dot(left, right, preferred_element_type=jnp.float32)


def data_by_table(values, table):
    high, low = split(values)
    return dot(high, table[0]) + dot(high, table[1]) + dot(low, table[0])


def table_by_data(table, values):
    high, low = split(values)
    return dot(table[0], high) + dot(table[1], high) + dot(table[0], low)


def local_kernel(psi_ref, wz_ref, wy_ref, out_ref):
    _, _, bx, ny, nz = psi_ref.shape
    grid_count, _, _, vy, _ = out_ref.shape
    real_part = psi_ref[0, 0].reshape(bx * ny, nz)
    imag_part = psi_ref[0, 1].reshape(bx * ny, nz)
    turned = data_by_table(jnp.concatenate([real_part, imag_part], 1), wz_ref)
    columns = [
        jnp.concatenate(
            [turned[p * ny : (p + 1) * ny, :nz], turned[p * ny : (p + 1) * ny, nz:]], 0
        )
        for p in range(bx)
    ]
    rows = table_by_data(wy_ref, jnp.concatenate(columns, 1))
    for g in range(grid_count):
        for c in range(2):
            start = c * ny + g * vy
            for p in range(bx):
                out_ref[g, c, p] = rows[start : start + vy, p * nz : (p + 1) * nz]


def kinetic_local(orbitals, layer, grid_count, wz, wy):
    _, _, planes, ny, nz = orbitals.shape
    bx = min(4, planes)
    vy = ny // grid_count
    return pl.pallas_call(
        local_kernel,
        grid=(planes // bx,),
        in_specs=[
            pl.BlockSpec((1, 2, bx, ny, nz), lambda i: (layer, 0, i, 0, 0)),
            pl.BlockSpec(wz.shape, lambda i: (0, 0, 0)),
            pl.BlockSpec(wy.shape, lambda i: (0, 0, 0)),
        ],
        out_specs=pl.BlockSpec((grid_count, 2, bx, vy, nz), lambda i: (0, 0, i, 0, 0)),
        out_shape=jax.ShapeDtypeStruct((grid_count, 2, planes, vy, nz), jnp.float32),
        compiler_params=pltpu.CompilerParams(vmem_limit_bytes=VMEM_LIMIT),
        cost_estimate=pl.CostEstimate(
            flops=3 * 8 * planes * ny * nz * (ny + nz),
            bytes_accessed=16 * planes * ny * nz,
            transcendentals=0,
        ),
    )(orbitals, wz, wy)


def across_kernel(planes, first, weight_ref, psi_ref, wx_ref, *refs):
    if first:
        out_ref, density_ref = refs
    else:
        earlier_ref, out_ref, density_ref = refs
    depth, by, nz = psi_ref.shape
    columns = jnp.concatenate([psi_ref[:, j, :] for j in range(by)], 1)
    moved = table_by_data(wx_ref, columns)
    squares = moved * moved
    weight = weight_ref[0]
    for j in range(by):
        out_ref[:, j, :] = moved[:, j * nz : (j + 1) * nz]
    for h in range(depth // (2 * planes)):
        low = 2 * h * planes
        term = weight * (squares[low : low + planes] + squares[low + planes : low + 2 * planes])
        for j in range(by):
            value = term[:, j * nz : (j + 1) * nz]
            if not first:
                value = value + earlier_ref[h * planes : (h + 1) * planes, j, :]
            density_ref[h * planes : (h + 1) * planes, j, :] = value


def kinetic_across(received, weight, density, wx):
    grid_count, _, planes, vy, nz = received.shape
    depth = grid_count * 2 * planes
    by = min(8, vy)
    first = density is None
    block = pl.BlockSpec((depth, by, nz), lambda i: (0, i, 0))
    density_block = pl.BlockSpec((depth // 2, by, nz), lambda i: (0, i, 0))
    in_specs = [
        pl.BlockSpec(memory_space=pltpu.SMEM),
        block,
        pl.BlockSpec(wx.shape, lambda i: (0, 0, 0)),
    ]
    operands = [weight, received.reshape(depth, vy, nz), wx]
    if not first:
        in_specs.append(density_block)
        operands.append(density)
    moved, density = pl.pallas_call(
        partial(across_kernel, planes, first),
        grid=(vy // by,),
        in_specs=in_specs,
        out_specs=[block, density_block],
        out_shape=[
            jax.ShapeDtypeStruct((depth, vy, nz), jnp.float32),
            jax.ShapeDtypeStruct((depth // 2, vy, nz), jnp.float32),
        ],
        compiler_params=pltpu.CompilerParams(vmem_limit_bytes=VMEM_LIMIT),
        cost_estimate=pl.CostEstimate(
            flops=3 * 2 * depth * depth * vy * nz,
            bytes_accessed=12 * depth * vy * nz,
            transcendentals=0,
        ),
    )(*operands)
    return moved.reshape(grid_count, 2, planes, vy, nz), density


LANE_ROWS = 8
MESH = pl.DeviceIdType.MESH
EPS = float(np.finfo(np.float32).eps)


def far_factors(block):
    block = block.astype(np.clongdouble)
    norm2 = np.sum(np.abs(block) ** 2)
    residual = block.copy()
    rank = 0
    basis = []
    for _ in range(block.shape[1]):
        sizes = np.sum(np.abs(residual) ** 2, axis=1)
        if np.sum(sizes) <= (EPS * EPS) * 1e-3 * norm2:
            break
        row = residual[int(np.argmax(sizes))].conj()
        for other in basis:
            row = row - other * np.sum(other.conj() * row)
        row = row / np.sqrt(np.sum(np.abs(row) ** 2))
        basis.append(row)
        residual = residual - np.sum(residual * row[None, :], axis=1)[:, None] * row.conj()[None, :]
    gram = np.matmul(block.conj().T, block)
    for _ in range(8):
        basis = [np.sum(gram * vector[None, :], axis=1) for vector in basis]
        clean = []
        for row in basis:
            for _ in range(2):
                for other in clean:
                    row = row - other * np.sum(other.conj() * row)
            clean.append(row / np.sqrt(np.sum(np.abs(row) ** 2)))
        basis = clean
    for rank in range(1, len(basis) + 1):
        right = np.stack(basis[:rank], 1)
        left = np.matmul(block, right)
        rest = block - np.matmul(left, right.conj().T)
        if np.linalg.norm(rest.astype(np.complex128), 2) <= EPS:
            break
    return left.astype(np.complex128), right.astype(np.complex128)


def real_form(matrix):
    return np.block([[matrix.real, -matrix.imag], [matrix.imag, matrix.real]])


def stacked_table(table):
    high, low = split_const(table).astype(np.float32)
    return np.block([[high, high], [low, np.zeros_like(low)]]).astype(ml_dtypes.bfloat16)


def evolve_tables(width_x, planes):
    matrix = kinetic_matrix(width_x)
    half = 2 * planes
    left, right = far_factors(matrix[half:, :half])
    rank = -(-left.shape[1] // 2) * 2
    pad = rank - left.shape[1]
    left = np.pad(left, ((0, 0), (0, pad)))
    right = np.pad(right, ((0, 0), (0, pad)))
    near = matrix[:planes, :planes]
    sides = []
    for core in range(2):
        mine = slice(core * planes, (core + 1) * planes)
        theirs = slice((1 - core) * planes, (2 - core) * planes)
        sides.append(
            (left[mine], right[mine], far_factors(matrix[theirs, mine]), far_factors(matrix[mine, theirs]))
        )
    core_rank = max(s[2][0].shape[1] for s in sides)
    core_rank = -(-core_rank // 4) * 4
    widen = lambda m: np.pad(m, ((0, 0), (0, core_rank - m.shape[1])))
    far = -(-2 * rank // 8) * 8
    gather, spread = [], []
    for mine_left, mine_right, (_, give), (take, _) in sides:
        rows = real_form(mine_right.conj().T)
        rows = np.concatenate([rows, np.zeros((far - rows.shape[0], rows.shape[1]))], 0)
        core_rows = real_form(widen(give).conj().T)
        gather.append(stacked_table(np.concatenate([rows, core_rows], 0)))
        far_columns = real_form(mine_left)
        far_columns = np.pad(far_columns, ((0, 0), (0, far - far_columns.shape[1])))
        spread.append(
            stacked_table(np.concatenate([real_form(near), real_form(widen(take)), far_columns], 1))
        )
    return np.stack(gather), np.stack(spread), 2 * rank, far, 2 * core_rank


def stack_split(values):
    high, low = split(values)
    return jnp.concatenate([high, low], 0)


def evolve_kernel(
    layers, far_rows, far, near_rows, lag,
    weight_ref, psi_ref, wz_ref, wy_ref, gather_ref, spread_ref,
    out_ref, density_ref,
    stage, phi, give_far, give_near, got_far, got_near, far_field, result, density,
    in_sem, out_sem, p_send, p_recv, q_send, q_recv, y_send, y_recv, f_send, f_recv, density_sem,
):
    _, _, planes, ny, nz = psi_ref.shape
    groups = ny // LANE_ROWS
    tiles = groups // 2
    units = layers * tiles
    bx = planes // tiles
    place = lax.axis_index("grid")
    core = lax.rem(place, 2)
    sibling = place + 1 - 2 * core
    across = lax.rem(place + 2, 4)

    def far_copy(unit):
        return pltpu.make_async_remote_copy(
            src_ref=give_far.at[lax.rem(unit, 4), 1 - core], dst_ref=got_far.at[unit],
            send_sem=p_send.at[unit], recv_sem=p_recv.at[unit],
            device_id={"grid": sibling}, device_id_type=MESH,
        )

    def near_copy(unit):
        return pltpu.make_async_remote_copy(
            src_ref=give_near.at[lax.rem(unit, 4)], dst_ref=got_near.at[unit],
            send_sem=q_send.at[unit], recv_sem=q_recv.at[unit],
            device_id={"grid": sibling}, device_id_type=MESH,
        )

    def across_copy(unit):
        return pltpu.make_async_remote_copy(
            src_ref=got_far.at[unit], dst_ref=far_field.at[unit, core, pl.ds(0, far_rows)],
            send_sem=y_send.at[unit], recv_sem=y_recv.at[unit],
            device_id={"grid": across}, device_id_type=MESH,
        )

    def share_copy(unit):
        held = far_field.at[unit, core, pl.ds(0, far_rows)]
        return pltpu.make_async_remote_copy(
            src_ref=held, dst_ref=held,
            send_sem=f_send.at[unit], recv_sem=f_recv.at[unit],
            device_id={"grid": sibling}, device_id_type=MESH,
        )

    def load_copy(step):
        layer, part = step // tiles, lax.rem(step, tiles)
        slot = lax.rem(step, 3)
        return pltpu.make_async_copy(
            psi_ref.at[layer, :, pl.ds(part * bx, bx)], stage.at[slot], in_sem.at[slot]
        )

    def result_copy(unit, half):
        layer, tile = unit // tiles, lax.rem(unit, tiles)
        slot = lax.rem(unit, 3)
        row = pl.multiple_of((2 * tile + half) * LANE_ROWS, LANE_ROWS)
        return pltpu.make_async_copy(
            result.at[slot, half],
            out_ref.at[layer, :, pl.ds(row, LANE_ROWS), :],
            out_sem.at[slot, half],
        )

    load_copy(0).start()
    load_copy(1).start()
    if far > far_rows:
        far_field[:, :, far_rows:] = jnp.zeros((units, 2, far - far_rows, LANE_ROWS, nz), jnp.float32)
    barrier = pltpu.get_barrier_semaphore()
    for peer in (sibling, across):
        pl.semaphore_signal(barrier, inc=1, device_id={"grid": peer}, device_id_type=MESH)
    pl.semaphore_wait(barrier, 2)

    def plane_step(step):
        @pl.when(step + 2 < units)
        def _():
            load_copy(step + 2).start()

        load_copy(step).wait()
        layer, part = step // tiles, lax.rem(step, tiles)
        slot = lax.rem(step, 3)
        real_part = stage[slot, 0].reshape(bx * ny, nz)
        imag_part = stage[slot, 1].reshape(bx * ny, nz)
        turned = data_by_table(jnp.concatenate([real_part, imag_part], 1), wz_ref)
        columns = [
            jnp.concatenate([turned[p * ny : (p + 1) * ny, :nz], turned[p * ny : (p + 1) * ny, nz:]], 0)
            for p in range(bx)
        ]
        rows = table_by_data(wy_ref, jnp.concatenate(columns, 1))
        for c in range(2):
            for p in range(bx):
                block = rows[c * ny : (c + 1) * ny, p * nz : (p + 1) * nz]
                phi[layer, :, c * planes + part * bx + p] = block.reshape(groups, LANE_ROWS, nz)

    def gather_step(unit):
        layer, tile = unit // tiles, lax.rem(unit, tiles)
        slot = lax.rem(unit, 4)

        @pl.when(unit >= 4)
        def _():
            far_copy(unit - 4).wait_send()
            near_copy(unit - 4).wait_send()

        for half in range(2):
            for part in range(2):
                ids = range(4 * part, 4 * part + 4)
                data = jnp.concatenate([phi[layer, 2 * tile + half, :, i, :] for i in ids], 1)
                both = dot(gather_ref[core], stack_split(data))
                total = both[: far + near_rows] + both[far + near_rows :]
                for k, i in enumerate(ids):
                    block = total[:, k * nz : (k + 1) * nz]
                    give_far[slot, half, :, i, :] = block[:far_rows]
                    give_near[slot, half, :, i, :] = block[far:]

    def sum_step(unit):
        far_copy(unit).wait_recv()
        got_far[unit] = got_far[unit] + give_far[lax.rem(unit, 4), core]

    def spread_step(unit):
        layer, tile = unit // tiles, lax.rem(unit, tiles)
        slot = lax.rem(unit, 3)
        near_copy(unit).wait_recv()
        share_copy(unit).wait_recv()

        @pl.when(unit >= 3)
        def _():
            result_copy(unit - 3, 0).wait()
            result_copy(unit - 3, 1).wait()

        weight = weight_ref[layer]
        for half in range(2):
            for part in range(2):
                ids = range(4 * part, 4 * part + 4)
                data = jnp.concatenate(
                    [
                        jnp.concatenate(
                            [
                                phi[layer, 2 * tile + half, :, i, :],
                                got_near[unit, half, :, i, :],
                                far_field[unit, half, :, i, :],
                            ],
                            0,
                        )
                        for i in ids
                    ],
                    1,
                )
                both = dot(spread_ref[core], stack_split(data))
                moved = both[: 2 * planes] + both[2 * planes :]
                squares = moved * moved
                term = weight * (squares[:planes] + squares[planes:])
                for k, i in enumerate(ids):
                    result[slot, half, :, i, :] = moved[:, k * nz : (k + 1) * nz]
                    earlier = density[2 * tile + half, :, i, :]
                    value = term[:, k * nz : (k + 1) * nz]
                    density[2 * tile + half, :, i, :] = value + jnp.where(layer == 0, 0.0, earlier)

    first_gather = tiles
    first_forward = tiles + 3 + lag
    first_spread = first_forward + 2

    def tick(t, carry):
        def stage_at(start, action):
            unit = t - start

            @pl.when((unit >= 0) & (unit < units))
            def _():
                action(unit)

        def send(unit):
            far_copy(unit).start()
            near_copy(unit).start()

        def forward(unit):
            across_copy(unit).wait_recv()
            share_copy(unit).start()

        def write(unit):
            result_copy(unit, 0).start()
            result_copy(unit, 1).start()

        stage_at(first_gather + 1, send)
        stage_at(first_gather + 3, lambda unit: across_copy(unit).start())
        stage_at(first_spread + 1, write)
        stage_at(0, plane_step)
        stage_at(first_gather + 2, sum_step)
        stage_at(first_gather, gather_step)
        stage_at(first_forward, forward)
        stage_at(first_spread, spread_step)
        return carry

    density[...] = jnp.zeros_like(density)
    lax.fori_loop(0, first_spread + 1 + units, tick, 0)

    for g in range(groups):
        pltpu.make_async_copy(
            density.at[g], density_ref.at[:, pl.ds(g * LANE_ROWS, LANE_ROWS), :], density_sem.at[g]
        ).start()

    def finish(unit, carry):
        across_copy(unit).wait_send()
        share_copy(unit).wait_send()

        @pl.when(unit >= units - 4)
        def _():
            far_copy(unit).wait_send()
            near_copy(unit).wait_send()

        @pl.when(unit >= units - 3)
        def _():
            result_copy(unit, 0).wait()
            result_copy(unit, 1).wait()

        return carry

    lax.fori_loop(0, units, finish, 0)
    for g in range(groups):
        pltpu.make_async_copy(
            density.at[g], density_ref.at[:, pl.ds(g * LANE_ROWS, LANE_ROWS), :], density_sem.at[g]
        ).wait()


def evolve(orbitals, weights, wz, wy):
    layers, _, planes, ny, nz = orbitals.shape
    gather, spread, far_rows, far, near_rows = evolve_tables(4 * planes, planes)
    groups = ny // LANE_ROWS
    units = layers * groups // 2
    f32 = jnp.float32
    vmem = pl.BlockSpec(memory_space=pltpu.VMEM)
    anywhere = pl.BlockSpec(memory_space=pl.ANY)
    dma = pltpu.SemaphoreType.DMA
    evolved, density = pl.pallas_call(
        partial(evolve_kernel, layers, far_rows, far, near_rows, 3),
        in_specs=[pl.BlockSpec(memory_space=pltpu.SMEM), anywhere, vmem, vmem, vmem, vmem],
        out_specs=[anywhere, anywhere],
        out_shape=[
            jax.ShapeDtypeStruct((layers, 2 * planes, ny, nz), f32),
            jax.ShapeDtypeStruct((planes, ny, nz), f32),
        ],
        scratch_shapes=[
            pltpu.VMEM((3, 2, planes * 2 // groups, ny, nz), f32),
            pltpu.VMEM((layers, groups, 2 * planes, LANE_ROWS, nz), f32),
            pltpu.VMEM((4, 2, far_rows, LANE_ROWS, nz), f32),
            pltpu.VMEM((4, 2, near_rows, LANE_ROWS, nz), f32),
            pltpu.VMEM((units, far_rows, LANE_ROWS, nz), f32),
            pltpu.VMEM((units, 2, near_rows, LANE_ROWS, nz), f32),
            pltpu.VMEM((units, 2, far, LANE_ROWS, nz), f32),
            pltpu.VMEM((3, 2, 2 * planes, LANE_ROWS, nz), f32),
            pltpu.VMEM((groups, planes, LANE_ROWS, nz), f32),
            dma((3,)),
            dma((3, 2)),
        ]
        + [dma((units,))] * 8
        + [dma((groups,))],
        compiler_params=pltpu.CompilerParams(
            vmem_limit_bytes=60 * 1024 * 1024, collective_id=0, has_side_effects=True
        ),
        cost_estimate=pl.CostEstimate(
            flops=40 * layers * planes * ny * nz * (ny + nz), bytes_accessed=16 * layers * planes * ny * nz, transcendentals=0
        ),
    )(weights, orbitals, wz, wy, jnp.asarray(gather), jnp.asarray(spread))
    return evolved.reshape(layers, 2, planes, ny, nz), density


def turn_kernel(psi_ref, cos_ref, sin_ref, out_ref):
    cosine, sine = cos_ref[...], sin_ref[...]
    for l in range(psi_ref.shape[0]):
        real_part, imag_part = psi_ref[l, 0], psi_ref[l, 1]
        out_ref[l, 0] = real_part * cosine + imag_part * sine
        out_ref[l, 1] = imag_part * cosine - real_part * sine


def turn(evolved, cosine, sine):
    layers, _, planes, ny, nz = evolved.shape
    bx = min(4, planes)
    field_block = pl.BlockSpec((bx, ny, nz), lambda i: (i, 0, 0))
    block = pl.BlockSpec((layers, 2, bx, ny, nz), lambda i: (0, 0, i, 0, 0))
    return pl.pallas_call(
        turn_kernel,
        grid=(planes // bx,),
        in_specs=[block, field_block, field_block],
        out_specs=block,
        out_shape=jax.ShapeDtypeStruct(evolved.shape, jnp.float32),
        compiler_params=pltpu.CompilerParams(vmem_limit_bytes=VMEM_LIMIT),
    )(evolved, cosine, sine)


def rotate_kernel(layers, *refs):
    cos_ref, sin_ref = refs[layers], refs[layers + 1]
    out_ref = refs[layers + 2]
    grid_count, _, _, vy, _ = refs[0].shape
    for g in range(grid_count):
        band = slice(g * vy, (g + 1) * vy)
        cosine = cos_ref[:, band, :]
        sine = sin_ref[:, band, :]
        for l in range(layers):
            real_part = refs[l][g, 0]
            imag_part = refs[l][g, 1]
            out_ref[l, 0, :, band, :] = real_part * cosine + imag_part * sine
            out_ref[l, 1, :, band, :] = imag_part * cosine - real_part * sine


def rotate(returned, cosine, sine):
    layers = len(returned)
    grid_count, _, planes, vy, nz = returned[0].shape
    ny = grid_count * vy
    bx = min(4, planes)
    field_block = pl.BlockSpec((bx, ny, nz), lambda i: (i, 0, 0))
    return pl.pallas_call(
        partial(rotate_kernel, layers),
        grid=(planes // bx,),
        in_specs=[pl.BlockSpec((grid_count, 2, bx, vy, nz), lambda i: (0, 0, i, 0, 0))] * layers
        + [field_block, field_block],
        out_specs=pl.BlockSpec((layers, 2, bx, ny, nz), lambda i: (0, 0, i, 0, 0)),
        out_shape=jax.ShapeDtypeStruct((layers, 2, planes, ny, nz), jnp.float32),
        compiler_params=pltpu.CompilerParams(vmem_limit_bytes=VMEM_LIMIT),
    )(*returned, cosine, sine)


def table_of(matrix):
    return (np.asarray(matrix.real, np.float32), np.asarray(matrix.imag, np.float32))


def apply_along(values, table, axis):
    contracted = jnp.tensordot(values, table, axes=([axis], [0]), precision=HIGHEST)
    return jnp.moveaxis(contracted, -1, axis)


def complex_along(real_part, imag_part, matrix, axis):
    table_re, table_im = table_of(matrix)
    new_re = apply_along(real_part, table_re, axis) - apply_along(imag_part, table_im, axis)
    new_im = apply_along(real_part, table_im, axis) + apply_along(imag_part, table_re, axis)
    return (new_re, new_im)


def coulomb_kernel(squares_x, squares_y, squares_z):
    total = squares_x[:, None, None] + squares_y[None, :, None] + squares_z[None, None, :]
    anchor = total <= 0.0
    return jnp.where(anchor, 0.0, HARTREE_SCALE / jnp.where(anchor, 1.0, total))


def poisson_shared(density, names):
    width_x, _, count_z = density.shape
    span_count = lax.axis_size("grid") * lax.axis_size("orb")
    block_x = width_x // span_count
    forward_z = table_of(fourier(count_z, -1))
    real_part, imag_part = (apply_along(density, forward_z[0], 2), apply_along(density, forward_z[1], 2))
    real_part, imag_part = complex_along(real_part, imag_part, fourier(width_x, -1), 0)
    spread = lax.all_to_all(
        jnp.stack([real_part, imag_part], 0),
        names,
        split_axis=1,
        concat_axis=2,
        tiled=True,
    )
    count_y = spread.shape[2]
    real_part, imag_part = complex_along(spread[0], spread[1], fourier(count_y, -1), 1)
    start_x = lax.axis_index(names) * block_x
    squares_x = lax.dynamic_slice_in_dim(
        jnp.asarray(wave_squared(width_x), jnp.float32), start_x, block_x, 0
    )
    kernel = coulomb_kernel(
        squares_x,
        np.asarray(wave_squared(count_y), np.float32),
        np.asarray(wave_squared(count_z), np.float32),
    )
    real_part, imag_part = complex_along(
        real_part * kernel, imag_part * kernel, fourier(count_y, 1) / count_y, 1
    )
    back = lax.all_to_all(
        jnp.stack([real_part, imag_part], 0),
        names,
        split_axis=2,
        concat_axis=1,
        tiled=True,
    )
    real_part, imag_part = complex_along(back[0], back[1], fourier(width_x, 1) / width_x, 0)
    inverse_z = table_of(fourier(count_z, 1) / count_z)
    return apply_along(real_part, inverse_z[0], 2) - apply_along(imag_part, inverse_z[1], 2)


def body(orbitals, v_local, occupations):
    layers, _, planes, count_y, count_z = orbitals.shape
    grid_count = lax.axis_size("grid")
    orb_count = lax.axis_size("orb")
    width_x = planes * grid_count
    share_y = count_y // (grid_count * orb_count)
    wz = jnp.asarray(split_const(right_block(kinetic_matrix(count_z))))
    wy = jnp.asarray(split_const(left_block(kinetic_matrix(count_y))))
    order = np.arange(2 * width_x).reshape(2, grid_count, planes).transpose(1, 0, 2).reshape(-1)
    wx = jnp.asarray(split_const(left_block(kinetic_matrix(width_x))[order][:, order]))
    weights = lax.dynamic_slice_in_dim(occupations, lax.axis_index("orb") * layers, layers, 0)
    if grid_count == 4 and 2 * planes % (count_y // LANE_ROWS) == 0 and count_y % (2 * LANE_ROWS) == 0:
        evolved, density = evolve(orbitals, weights, wz, wy)
        share = lax.psum_scatter(density, "orb", scatter_dimension=1, tiled=True)
        lines = lax.all_to_all(share, "grid", split_axis=1, concat_axis=0, tiled=True)
        hartree_lines = poisson_shared(lines, ("orb", "grid"))
        rows_back = lax.all_to_all(hartree_lines, "grid", split_axis=0, concat_axis=1, tiled=True)
        hartree = lax.all_gather(rows_back, "orb", axis=1, tiled=True)
        angle = TIME_STEP * (v_local + hartree)
        return turn(evolved, jnp.cos(angle), jnp.sin(angle))
    exchange = partial(lax.all_to_all, axis_name="grid", split_axis=0, concat_axis=0, tiled=True)

    received = [
        exchange(kinetic_local(orbitals, layer, grid_count, wz, wy)) for layer in range(layers)
    ]
    density = None
    returned = []
    for layer in range(layers):
        moved, density = kinetic_across(
            received[layer], weights[layer : layer + 1], density, wx
        )
        returned.append(exchange(moved))
    share = lax.psum_scatter(density, "orb", scatter_dimension=1, tiled=True)
    share, returned[0] = lax.optimization_barrier((share, returned[0]))
    hartree_lines = poisson_shared(share, ("grid", "orb"))
    rows_back = lax.all_to_all(hartree_lines, "grid", split_axis=0, concat_axis=1, tiled=True)
    gathered = lax.all_gather(rows_back, "orb", axis=0, tiled=False)
    hartree = gathered.reshape(orb_count, planes, grid_count, share_y, count_z)
    hartree = hartree.transpose(1, 2, 0, 3, 4).reshape(planes, count_y, count_z)
    angle = TIME_STEP * (v_local + hartree)
    return rotate(returned, jnp.cos(angle), jnp.sin(angle))


def solution(mesh):
    return jax.shard_map(
        body,
        mesh=mesh,
        in_specs=(
            P(("groups", "orb"), None, "grid", None, None),
            P(("groups", "grid"), None, None),
            P("groups"),
        ),
        out_specs=P(("groups", "orb"), None, "grid", None, None),
        check_vma=False,
    )
```

```python
from functools import partial
import math

import jax
import jax.numpy as jnp
import ml_dtypes
import numpy as np
from jax import lax
from jax.experimental import pallas as pl
from jax.experimental.pallas import tpu as pltpu
from jax.sharding import PartitionSpec as P

TIME_STEP = 0.05
KINETIC_RATE = 0.1
HARTREE_SCALE = math.pi
HIGHEST = lax.Precision.HIGHEST
VMEM_LIMIT = 50 * 1024 * 1024


def wave_squared(length):
    ids = np.arange(length)
    signed = np.where(ids < (length + 1) // 2, ids, ids - length)
    return (2.0 * np.pi * signed / length) ** 2


def fourier(length, sign):
    ids = np.arange(length)
    return np.exp(sign * 2j * np.pi * ((ids[:, None] * ids[None, :]) % length) / length)


def kinetic_matrix(length):
    phase = np.exp(-1j * KINETIC_RATE * wave_squared(length))
    return (fourier(length, 1) / length * phase[None, :]) @ fourier(length, -1)


def left_block(matrix):
    return np.block([[matrix.real, -matrix.imag], [matrix.imag, matrix.real]])


def right_block(matrix):
    return np.block([[matrix.real, matrix.imag], [-matrix.imag, matrix.real]])


def split_const(table):
    table = np.asarray(table, np.float32)
    high = table.astype(ml_dtypes.bfloat16)
    low = (table - high.astype(np.float32)).astype(ml_dtypes.bfloat16)
    return np.stack([high, low])


def split(values):
    high = values.astype(jnp.bfloat16)
    low = (values - high.astype(jnp.float32)).astype(jnp.bfloat16)
    return high, low


def dot(left, right):
    return jnp.dot(left, right, preferred_element_type=jnp.float32)


def data_by_table(values, table):
    high, low = split(values)
    return dot(high, table[0]) + dot(high, table[1]) + dot(low, table[0])


def table_by_data(table, values):
    high, low = split(values)
    return dot(table[0], high) + dot(table[1], high) + dot(table[0], low)


def local_kernel(psi_ref, wz_ref, wy_ref, out_ref):
    _, _, bx, ny, nz = psi_ref.shape
    grid_count, _, _, vy, _ = out_ref.shape
    real_part = psi_ref[0, 0].reshape(bx * ny, nz)
    imag_part = psi_ref[0, 1].reshape(bx * ny, nz)
    turned = data_by_table(jnp.concatenate([real_part, imag_part], 1), wz_ref)
    columns = [
        jnp.concatenate(
            [turned[p * ny : (p + 1) * ny, :nz], turned[p * ny : (p + 1) * ny, nz:]], 0
        )
        for p in range(bx)
    ]
    rows = table_by_data(wy_ref, jnp.concatenate(columns, 1))
    for g in range(grid_count):
        for c in range(2):
            start = c * ny + g * vy
            for p in range(bx):
                out_ref[g, c, p] = rows[start : start + vy, p * nz : (p + 1) * nz]


def kinetic_local(orbitals, layer, grid_count, wz, wy):
    _, _, planes, ny, nz = orbitals.shape
    bx = min(4, planes)
    vy = ny // grid_count
    return pl.pallas_call(
        local_kernel,
        grid=(planes // bx,),
        in_specs=[
            pl.BlockSpec((1, 2, bx, ny, nz), lambda i: (layer, 0, i, 0, 0)),
            pl.BlockSpec(wz.shape, lambda i: (0, 0, 0)),
            pl.BlockSpec(wy.shape, lambda i: (0, 0, 0)),
        ],
        out_specs=pl.BlockSpec((grid_count, 2, bx, vy, nz), lambda i: (0, 0, i, 0, 0)),
        out_shape=jax.ShapeDtypeStruct((grid_count, 2, planes, vy, nz), jnp.float32),
        compiler_params=pltpu.CompilerParams(vmem_limit_bytes=VMEM_LIMIT),
        cost_estimate=pl.CostEstimate(
            flops=3 * 8 * planes * ny * nz * (ny + nz),
            bytes_accessed=16 * planes * ny * nz,
            transcendentals=0,
        ),
    )(orbitals, wz, wy)


def across_kernel(planes, first, weight_ref, psi_ref, wx_ref, *refs):
    if first:
        out_ref, density_ref = refs
    else:
        earlier_ref, out_ref, density_ref = refs
    depth, by, nz = psi_ref.shape
    columns = jnp.concatenate([psi_ref[:, j, :] for j in range(by)], 1)
    moved = table_by_data(wx_ref, columns)
    squares = moved * moved
    weight = weight_ref[0]
    for j in range(by):
        out_ref[:, j, :] = moved[:, j * nz : (j + 1) * nz]
    for h in range(depth // (2 * planes)):
        low = 2 * h * planes
        term = weight * (squares[low : low + planes] + squares[low + planes : low + 2 * planes])
        for j in range(by):
            value = term[:, j * nz : (j + 1) * nz]
            if not first:
                value = value + earlier_ref[h * planes : (h + 1) * planes, j, :]
            density_ref[h * planes : (h + 1) * planes, j, :] = value


def kinetic_across(received, weight, density, wx):
    grid_count, _, planes, vy, nz = received.shape
    depth = grid_count * 2 * planes
    by = min(8, vy)
    first = density is None
    block = pl.BlockSpec((depth, by, nz), lambda i: (0, i, 0))
    density_block = pl.BlockSpec((depth // 2, by, nz), lambda i: (0, i, 0))
    in_specs = [
        pl.BlockSpec(memory_space=pltpu.SMEM),
        block,
        pl.BlockSpec(wx.shape, lambda i: (0, 0, 0)),
    ]
    operands = [weight, received.reshape(depth, vy, nz), wx]
    if not first:
        in_specs.append(density_block)
        operands.append(density)
    moved, density = pl.pallas_call(
        partial(across_kernel, planes, first),
        grid=(vy // by,),
        in_specs=in_specs,
        out_specs=[block, density_block],
        out_shape=[
            jax.ShapeDtypeStruct((depth, vy, nz), jnp.float32),
            jax.ShapeDtypeStruct((depth // 2, vy, nz), jnp.float32),
        ],
        compiler_params=pltpu.CompilerParams(vmem_limit_bytes=VMEM_LIMIT),
        cost_estimate=pl.CostEstimate(
            flops=3 * 2 * depth * depth * vy * nz,
            bytes_accessed=12 * depth * vy * nz,
            transcendentals=0,
        ),
    )(*operands)
    return moved.reshape(grid_count, 2, planes, vy, nz), density


LANE_ROWS = 8
MESH = pl.DeviceIdType.MESH
EPS = float(np.finfo(np.float32).eps)


def far_factors(block):
    block = block.astype(np.clongdouble)
    norm2 = np.sum(np.abs(block) ** 2)
    residual = block.copy()
    rank = 0
    basis = []
    for _ in range(block.shape[1]):
        sizes = np.sum(np.abs(residual) ** 2, axis=1)
        if np.sum(sizes) <= (EPS * EPS) * 1e-3 * norm2:
            break
        row = residual[int(np.argmax(sizes))].conj()
        for other in basis:
            row = row - other * np.sum(other.conj() * row)
        row = row / np.sqrt(np.sum(np.abs(row) ** 2))
        basis.append(row)
        residual = residual - np.sum(residual * row[None, :], axis=1)[:, None] * row.conj()[None, :]
    gram = np.matmul(block.conj().T, block)
    for _ in range(8):
        basis = [np.sum(gram * vector[None, :], axis=1) for vector in basis]
        clean = []
        for row in basis:
            for _ in range(2):
                for other in clean:
                    row = row - other * np.sum(other.conj() * row)
            clean.append(row / np.sqrt(np.sum(np.abs(row) ** 2)))
        basis = clean
    for rank in range(1, len(basis) + 1):
        right = np.stack(basis[:rank], 1)
        left = np.matmul(block, right)
        rest = block - np.matmul(left, right.conj().T)
        if np.linalg.norm(rest.astype(np.complex128), 2) <= EPS:
            break
    return left.astype(np.complex128), right.astype(np.complex128)


def real_form(matrix):
    return np.block([[matrix.real, -matrix.imag], [matrix.imag, matrix.real]])


def stacked_table(table):
    high, low = split_const(table).astype(np.float32)
    return np.block([[high, high], [low, np.zeros_like(low)]]).astype(ml_dtypes.bfloat16)


def evolve_tables(width_x, planes):
    matrix = kinetic_matrix(width_x)
    half = 2 * planes
    left, right = far_factors(matrix[half:, :half])
    rank = -(-left.shape[1] // 2) * 2
    pad = rank - left.shape[1]
    left = np.pad(left, ((0, 0), (0, pad)))
    right = np.pad(right, ((0, 0), (0, pad)))
    near = matrix[:planes, :planes]
    sides = []
    for core in range(2):
        mine = slice(core * planes, (core + 1) * planes)
        theirs = slice((1 - core) * planes, (2 - core) * planes)
        sides.append(
            (left[mine], right[mine], far_factors(matrix[theirs, mine]), far_factors(matrix[mine, theirs]))
        )
    core_rank = max(s[2][0].shape[1] for s in sides)
    core_rank = -(-core_rank // 4) * 4
    widen = lambda m: np.pad(m, ((0, 0), (0, core_rank - m.shape[1])))
    far = -(-2 * rank // 8) * 8
    gather, spread = [], []
    for mine_left, mine_right, (_, give), (take, _) in sides:
        rows = real_form(mine_right.conj().T)
        rows = np.concatenate([rows, np.zeros((far - rows.shape[0], rows.shape[1]))], 0)
        core_rows = real_form(widen(give).conj().T)
        gather.append(stacked_table(np.concatenate([rows, core_rows], 0)))
        far_columns = real_form(mine_left)
        far_columns = np.pad(far_columns, ((0, 0), (0, far - far_columns.shape[1])))
        spread.append(
            stacked_table(np.concatenate([real_form(near), real_form(widen(take)), far_columns], 1))
        )
    return np.stack(gather), np.stack(spread), 2 * rank, far, 2 * core_rank


def stack_split(values):
    high, low = split(values)
    return jnp.concatenate([high, low], 0)


def split_three(values):
    high = values.astype(jnp.bfloat16)
    rest = values - high.astype(jnp.float32)
    middle = rest.astype(jnp.bfloat16)
    low = (rest - middle.astype(jnp.float32)).astype(jnp.bfloat16)
    return [high, middle, low]


def six_table(table):
    parts, rest = [], np.asarray(table, np.float32)
    for _ in range(3):
        parts.append(rest.astype(ml_dtypes.bfloat16).astype(np.float32))
        rest = rest - parts[-1]
    high, middle, low = parts
    return np.concatenate([high, high, high, middle, middle, low], 1).astype(ml_dtypes.bfloat16)


def six_parts(values):
    high, middle, low = split_three(values)
    return [high, middle, low, high, middle, high]


def exact_left(table_ref, values):
    return dot(table_ref[...], jnp.concatenate(six_parts(values), 0))


def exact_right(values, table_ref):
    parts = six_parts(values)
    width = values.shape[1]
    total = None
    for pair in range(3):
        data = jnp.concatenate(parts[2 * pair : 2 * pair + 2], 1)
        term = dot(data, table_ref[2 * pair * width : 2 * (pair + 1) * width, :])
        total = term if total is None else total + term
    return total


def real_basis(length):
    ids = np.arange(length)
    angle = 2.0 * np.pi * ((ids[:, None] * ids[None, :]) % length) / length
    table = np.where(ids[None, :] <= length // 2, np.cos(angle), np.sin(angle))
    single = (ids == 0) | (2 * ids == length)
    return table * np.where(single, 1.0, math.sqrt(2.0))[None, :] / math.sqrt(length)


def rows_at(ref, row):
    return ref[pl.ds(row, ref.shape[0] // LANE_ROWS, stride=LANE_ROWS), :]


def put_rows(ref, row, values):
    ref[pl.ds(row, ref.shape[0] // LANE_ROWS, stride=LANE_ROWS), :] = values


def tile_of(index):
    return pl.ds(pl.multiple_of(index * LANE_ROWS, LANE_ROWS), LANE_ROWS)


def evolve_kernel(
    layers, far_rows, far, near_rows, lag,
    weight_ref, wave_ref, psi_ref, local_ref, wz_ref, wy_ref, gather_ref, spread_ref,
    qz_ref, qzt_ref, qy_ref, qyt_ref, qx_ref, qxt_ref, plane_wave_ref,
    out_ref, angle_ref,
    stage, phi, give_far, give_near, got_far, got_near, far_field, result, density,
    outer_sum, middle_sum, total, spectrum, lines, returned, local,
    in_sem, out_sem, p_send, p_recv, q_send, q_recv, y_send, y_recv, f_send, f_recv,
    a_send, a_recv, m_send, m_recv, t_send, t_recv, l_send, l_recv, b_send, b_recv, d_send, d_recv, v_sem,
):
    _, _, planes, ny, nz = psi_ref.shape
    groups = ny // LANE_ROWS
    tiles = groups // 2
    units = layers * tiles
    bx = stage.shape[2]
    per_layer = planes // bx
    steps = layers * per_layer
    paired = (layers - 3) * tiles
    place = lax.axis_index("grid")
    core = lax.rem(place, 2)
    sibling = place + 1 - 2 * core
    across = lax.rem(place + 2, 4)
    depth = lax.axis_index("orb")
    outer = (depth == 0) | (depth == 3)
    inner = (depth == 1) | (depth == 2)
    toward = 1 + depth // 3
    outward = jnp.where(depth == 1, 0, 3)
    middle = jnp.where(depth == 1, 2, 1)

    def where_is(unit):
        late = unit - paired
        layer = jnp.where(late < 0, unit // tiles, layers - 3 + lax.rem(jnp.maximum(late, 0), 3))
        tile = jnp.where(late < 0, lax.rem(unit, tiles), jnp.maximum(late, 0) // 3)
        return layer, tile

    def remote(source, target, send_sem, recv_sem, device):
        return pltpu.make_async_remote_copy(
            src_ref=source, dst_ref=target, send_sem=send_sem, recv_sem=recv_sem,
            device_id=device, device_id_type=MESH,
        )

    def far_copy(unit):
        return remote(
            give_far.at[lax.rem(unit, 4), 1 - core], got_far.at[unit],
            p_send.at[unit], p_recv.at[unit], {"grid": sibling},
        )

    def near_copy(unit):
        return remote(
            give_near.at[lax.rem(unit, 4)], got_near.at[unit],
            q_send.at[unit], q_recv.at[unit], {"grid": sibling},
        )

    def across_copy(unit):
        return remote(
            got_far.at[unit], far_field.at[unit, core, pl.ds(0, far_rows * LANE_ROWS)],
            y_send.at[unit], y_recv.at[unit], {"grid": across},
        )

    def share_copy(unit):
        held = far_field.at[unit, core, pl.ds(0, far_rows * LANE_ROWS)]
        return remote(held, held, f_send.at[unit], f_recv.at[unit], {"grid": sibling})

    def outer_copy(g):
        return remote(density.at[g], outer_sum.at[g], a_send.at[g], a_recv.at[g], {"orb": toward})

    def middle_copy(g):
        return remote(density.at[g], middle_sum.at[g], m_send.at[g], m_recv.at[g], {"orb": middle})

    def total_copy(g):
        return remote(total.at[g], total.at[g], t_send.at[g], t_recv.at[g], {"orb": outward})

    def load_copy(step):
        layer, part = step // per_layer, lax.rem(step, per_layer)
        slot = lax.rem(step, 3)
        return pltpu.make_async_copy(
            psi_ref.at[layer, :, pl.ds(part * bx, bx)], stage.at[slot], in_sem.at[slot]
        )

    def result_copy(unit, half):
        layer, tile = where_is(unit)
        slot = lax.rem(unit, 3)
        return pltpu.make_async_copy(
            result.at[slot, half],
            out_ref.at[layer, 2 * tile + half],
            out_sem.at[slot, half],
        )

    load_copy(0).start()
    load_copy(1).start()
    local_copy = pltpu.make_async_copy(local_ref, local, v_sem)
    local_copy.start()
    if far > far_rows:
        far_field[:, :, far_rows * LANE_ROWS :] = jnp.zeros((units, 2, (far - far_rows) * LANE_ROWS, nz), jnp.float32)
    density[...] = jnp.zeros_like(density)
    barrier = pltpu.get_barrier_semaphore()
    for k in range(1, 4):
        pl.semaphore_signal(barrier, inc=1, device_id={"grid": lax.rem(place + k, 4)}, device_id_type=MESH)

    @pl.when(outer)
    def _():
        pl.semaphore_signal(barrier, inc=1, device_id={"orb": toward}, device_id_type=MESH)
        pl.semaphore_wait(barrier, 4)

    @pl.when(inner)
    def _():
        pl.semaphore_signal(barrier, inc=1, device_id={"orb": outward}, device_id_type=MESH)
        pl.semaphore_signal(barrier, inc=1, device_id={"orb": middle}, device_id_type=MESH)
        pl.semaphore_wait(barrier, 5)

    def plane_step(step, carry):
        @pl.when(step + 2 < steps)
        def _():
            load_copy(step + 2).start()

        load_copy(step).wait()
        layer, part = step // per_layer, lax.rem(step, per_layer)
        slot = lax.rem(step, 3)
        real_part = stage[slot, 0].reshape(bx * ny, nz)
        imag_part = stage[slot, 1].reshape(bx * ny, nz)
        turned = data_by_table(jnp.concatenate([real_part, imag_part], 1), wz_ref)
        columns = [
            jnp.concatenate([turned[p * ny : (p + 1) * ny, :nz], turned[p * ny : (p + 1) * ny, nz:]], 0)
            for p in range(bx)
        ]
        rows = table_by_data(wy_ref, jnp.concatenate(columns, 1))
        for c in range(2):
            for p in range(bx):
                block = rows[c * ny : (c + 1) * ny, p * nz : (p + 1) * nz]
                phi[layer, :, tile_of(c * planes + part * bx + p), :] = block.reshape(groups, LANE_ROWS, nz)
        return carry

    def gather_step(unit):
        layer, tile = where_is(unit)
        slot = lax.rem(unit, 4)

        @pl.when(unit >= 4)
        def _():
            far_copy(unit - 4).wait_send()
            near_copy(unit - 4).wait_send()

        for half in range(2):
            for part in range(2):
                ids = range(4 * part, 4 * part + 4)
                source = phi.at[layer, 2 * tile + half]
                data = jnp.concatenate([rows_at(source, i) for i in ids], 1)
                both = dot(gather_ref[core], stack_split(data))
                joined = both[: far + near_rows] + both[far + near_rows :]
                for k, i in enumerate(ids):
                    block = joined[:, k * nz : (k + 1) * nz]
                    put_rows(give_far.at[slot, half], i, block[:far_rows])
                    put_rows(give_near.at[slot, half], i, block[far:])

    def sum_step(unit):
        far_copy(unit).wait_recv()
        got_far[unit] = got_far[unit] + give_far[lax.rem(unit, 4), core]

    def spread_step(unit):
        layer, tile = where_is(unit)
        slot = lax.rem(unit, 3)
        near_copy(unit).wait_recv()
        share_copy(unit).wait_recv()

        @pl.when(unit >= 3)
        def _():
            result_copy(unit - 3, 0).wait()
            result_copy(unit - 3, 1).wait()

        weight = weight_ref[layer]
        for half in range(2):
            for part in range(2):
                ids = range(4 * part, 4 * part + 4)
                data = jnp.concatenate(
                    [
                        jnp.concatenate(
                            [
                                rows_at(phi.at[layer, 2 * tile + half], i),
                                rows_at(got_near.at[unit, half], i),
                                rows_at(far_field.at[unit, half], i),
                            ],
                            0,
                        )
                        for i in ids
                    ],
                    1,
                )
                both = dot(spread_ref[core], stack_split(data))
                moved = both[: 2 * planes] + both[2 * planes :]
                squares = moved * moved
                term = weight * (squares[:planes] + squares[planes:])
                for k, i in enumerate(ids):
                    put_rows(result.at[slot, half], i, moved[:, k * nz : (k + 1) * nz])
                    summed = density.at[2 * tile + half]
                    put_rows(summed, i, rows_at(summed, i) + term[:, k * nz : (k + 1) * nz])

    def send(unit):
        far_copy(unit).start()
        near_copy(unit).start()

    def forward(unit):
        across_copy(unit).wait_recv()
        share_copy(unit).start()

    def write(unit):
        result_copy(unit, 0).start()
        result_copy(unit, 1).start()

    def add_outer(g):
        outer_copy(g).wait_recv()
        density[g] = density[g] + outer_sum[g]

    def add_middle(g):
        middle_copy(g).wait_recv()
        total[g] = density[g] + middle_sum[g]

    def flatten(g):
        outer_sum[g] = exact_right(total[g], qz_ref)

    def receive(g):
        total_copy(g).wait_recv()
        flatten(g)

    def prepared(t):
        late = jnp.maximum(t - 2, 0)
        return jnp.minimum(per_layer + (late * (layers - 1) * per_layer) // (paired - 2), steps)

    first_forward = 3 + lag
    first_spread = first_forward + 2
    ready = first_spread + 1
    last = ready + 15

    def tick(t, carry):
        def stage_at(start, action):
            unit = t - start

            @pl.when((unit >= 0) & (unit < units))
            def _():
                action(unit)

        def reduce_at(start, who, action):
            late = t - start - paired

            @pl.when((late >= 0) & (late < 3 * tiles) & (lax.rem(late + 3 * units, 3) == 2) & who)
            def _():
                action(2 * (late // 3))
                action(2 * (late // 3) + 1)

        stage_at(1, send)
        stage_at(3, lambda unit: across_copy(unit).start())
        stage_at(ready, write)
        reduce_at(ready, outer, lambda g: outer_copy(g).start())
        reduce_at(ready + 4, inner, add_outer)
        reduce_at(ready + 5, inner, lambda g: middle_copy(g).start())
        reduce_at(ready + 9, inner, add_middle)
        reduce_at(ready + 10, inner, lambda g: total_copy(g).start())
        reduce_at(ready + 10, inner, flatten)
        reduce_at(ready + 15, outer, receive)
        lax.fori_loop(prepared(t), prepared(t + 1), plane_step, 0)
        stage_at(2, sum_step)
        stage_at(0, gather_step)
        stage_at(first_forward, forward)
        stage_at(first_spread, spread_step)
        return carry

    lax.fori_loop(0, per_layer, plane_step, 0)
    lax.fori_loop(0, last + units, tick, 0)

    local_copy.wait()

    four = 4

    def spectrum_step(part, carry):
        ids = [part * four + p for p in range(four)]
        moved = exact_left(
            qyt_ref, jnp.concatenate([outer_sum[:, tile_of(x), :].reshape(ny, nz) for x in ids], 1)
        )
        for p, x in enumerate(ids):
            spectrum[:, tile_of(x), :] = moved[:, p * nz : (p + 1) * nz].reshape(groups, LANE_ROWS, nz)
        return carry

    lax.fori_loop(0, planes // four, spectrum_step, 0)
    share = groups // 8
    span = planes * LANE_ROWS
    mine = lax.rem(depth, 2) * (groups // 2)
    other = groups // 2 - mine
    partner = depth + 1 - 2 * lax.rem(depth, 2)

    def lines_of(device):
        return pl.ds(pl.multiple_of(device * span, span), span)

    def line_copy(g, k):
        peer = lax.rem(place + k, 4)
        return remote(
            spectrum.at[mine + peer * share + g], lines.at[g, lines_of(place)],
            l_send.at[g, k - 1], l_recv.at[g, k - 1], {"grid": peer},
        )

    def back_copy(g, k):
        peer = lax.rem(place + k, 4)
        return remote(
            lines.at[g, lines_of(peer)], returned.at[mine + place * share + g],
            b_send.at[g, k - 1], b_recv.at[g, k - 1], {"grid": peer},
        )

    def pair_copy(row):
        return remote(
            returned.at[row], returned.at[row],
            d_send.at[row], d_recv.at[row], {"orb": partner},
        )

    for g in range(share):
        for k in (2, 3, 1):
            line_copy(g, k).start()
        lines[g, lines_of(place)] = spectrum[mine + place * share + g]

    for g in range(share):
        for k in (1, 2, 3):
            line_copy(g, k).wait_recv()
        for part in range(2):
            ids = range(4 * part, 4 * part + 4)
            data = jnp.concatenate([rows_at(lines.at[g], i) for i in ids], 1)
            modes = exact_left(qxt_ref, data)
            scaled = []
            for k, i in enumerate(ids):
                waves = plane_wave_ref[...] + wave_ref[(mine + place * share + g) * LANE_ROWS + i]
                anchor = waves <= 0.0
                kernel = jnp.where(anchor, 0.0, HARTREE_SCALE / jnp.where(anchor, 1.0, waves))
                scaled.append(modes[:, k * nz : (k + 1) * nz] * kernel)
            moved = exact_left(qx_ref, jnp.concatenate(scaled, 1))
            for k, i in enumerate(ids):
                put_rows(lines.at[g], i, moved[:, k * nz : (k + 1) * nz])
        if g > 0:
            for k in (2, 3, 1):
                back_copy(g - 1, k).start()
    for k in (2, 3, 1):
        back_copy(share - 1, k).start()
    for g in range(share):
        returned[mine + place * share + g] = lines[g, lines_of(place)]
    for g in range(share):
        for k in (1, 2, 3):
            line_copy(g, k).wait_send()

    def straighten(row):
        spectrum[row] = exact_right(returned[row], qzt_ref)

    for g in range(share):
        pair_copy(mine + place * share + g).start()
    for g in range(share):
        straighten(mine + place * share + g)
    for g in range(share):
        for k in (3, 1, 2):
            row = mine + lax.rem(place + 4 - k, 4) * share + g
            back_copy(g, k).wait_recv()
            pair_copy(row).start()
            straighten(row)

    def finish(unit, carry):
        across_copy(unit).wait_send()
        share_copy(unit).wait_send()

        @pl.when(unit >= units - 4)
        def _():
            far_copy(unit).wait_send()
            near_copy(unit).wait_send()

        @pl.when(unit >= units - 3)
        def _():
            result_copy(unit, 0).wait()
            result_copy(unit, 1).wait()

        return carry

    lax.fori_loop(0, units, finish, 0)

    @pl.when(outer)
    def _():
        for g in range(groups):
            outer_copy(g).wait_send()

    @pl.when(inner)
    def _():
        for g in range(groups):
            middle_copy(g).wait_send()
            total_copy(g).wait_send()

    for k in (0, 3, 1, 2):
        for g in range(share):
            row = other + lax.rem(place + 4 - k, 4) * share + g
            pair_copy(row).wait_recv()
            straighten(row)

    def potential_step(part, carry):
        ids = [part * four + p for p in range(four)]
        moved = exact_left(
            qy_ref, jnp.concatenate([spectrum[:, tile_of(x), :].reshape(ny, nz) for x in ids], 1)
        )
        for p, x in enumerate(ids):
            angle_ref[x] = TIME_STEP * (local[x] + moved[:, p * nz : (p + 1) * nz])
        return carry

    lax.fori_loop(0, planes // four, potential_step, 0)
    for g in range(share):
        for k in (1, 2, 3):
            back_copy(g, k).wait_send()

    def settle(row, carry):
        pair_copy(mine + row).wait_send()
        return carry

    lax.fori_loop(0, groups // 2, settle, 0)


def evolve(orbitals, v_local, weights, wz, wy):
    layers, _, planes, ny, nz = orbitals.shape
    width_x = 4 * planes
    gather, spread, far_rows, far, near_rows = evolve_tables(width_x, planes)
    groups = ny // LANE_ROWS
    tiles = groups // 2
    units = layers * tiles
    f32 = jnp.float32
    squares = [wave_squared(n).astype(np.float32) for n in (width_x, ny, nz)]
    plane_wave = squares[0][:, None] + squares[2][None, :]
    basis = [real_basis(n) for n in (width_x, ny, nz)]
    tables = [
        six_table(basis[2].T).T, six_table(basis[2]).T, six_table(basis[1]), six_table(basis[1].T),
        six_table(basis[0]), six_table(basis[0].T), plane_wave,
    ]
    vmem = pl.BlockSpec(memory_space=pltpu.VMEM)
    smem = pl.BlockSpec(memory_space=pltpu.SMEM)
    anywhere = pl.BlockSpec(memory_space=pl.ANY)
    dma = pltpu.SemaphoreType.DMA
    field = pltpu.VMEM((groups, planes * LANE_ROWS, nz), f32)
    evolved, angle = pl.pallas_call(
        partial(evolve_kernel, layers, far_rows, far, near_rows, 3),
        in_specs=[smem, smem, anywhere, anywhere] + [vmem] * 11,
        out_specs=[anywhere, vmem],
        out_shape=[
            jax.ShapeDtypeStruct((layers, groups, 2 * planes * LANE_ROWS, nz), f32),
            jax.ShapeDtypeStruct((planes, ny, nz), f32),
        ],
        scratch_shapes=[
            pltpu.VMEM((3, 2, 8, ny, nz), f32),
            pltpu.VMEM((layers, groups, 2 * planes * LANE_ROWS, nz), f32),
            pltpu.VMEM((4, 2, far_rows * LANE_ROWS, nz), f32),
            pltpu.VMEM((4, 2, near_rows * LANE_ROWS, nz), f32),
            pltpu.VMEM((units, far_rows * LANE_ROWS, nz), f32),
            pltpu.VMEM((units, 2, near_rows * LANE_ROWS, nz), f32),
            pltpu.VMEM((units, 2, far * LANE_ROWS, nz), f32),
            pltpu.VMEM((3, 2, 2 * planes * LANE_ROWS, nz), f32),
            field, field, field, field, field,
            pltpu.VMEM((groups // 8, width_x * LANE_ROWS, nz), f32),
            field,
            pltpu.VMEM((planes, ny, nz), f32),
            dma((3,)),
            dma((3, 2)),
        ]
        + [dma((units,))] * 8
        + [dma((groups,))] * 6
        + [dma((groups // 8, 3))] * 4
        + [dma((groups,))] * 2
        + [pltpu.SemaphoreType.DMA],
        compiler_params=pltpu.CompilerParams(
            vmem_limit_bytes=63 * 1024 * 1024, collective_id=0, has_side_effects=True
        ),
        cost_estimate=pl.CostEstimate(
            flops=40 * layers * planes * ny * nz * (ny + nz), bytes_accessed=16 * layers * planes * ny * nz, transcendentals=0
        ),
    )(weights, jnp.asarray(squares[1]), orbitals, v_local, wz, wy, *map(jnp.asarray, [gather, spread] + tables))
    return evolved.reshape(layers, groups, 2, planes, LANE_ROWS, nz), angle


def cos_sin(angle):
    turns = jnp.floor(angle * (2.0 / math.pi) + 0.5)
    rest = ((angle - turns * 1.5703125) - turns * 4.837512969970703125e-4) - turns * 7.549789954891882e-8
    square = rest * rest
    sine = ((-1.9515295891e-4 * square + 8.3321608736e-3) * square - 1.6666654611e-1) * square * rest + rest
    cosine = (
        (2.443315711809948e-5 * square - 1.388731625493765e-3) * square + 4.166664568298827e-2
    ) * square * square - 0.5 * square + 1.0
    quarter = turns.astype(jnp.int32) & 3
    odd = (quarter & 1) == 1
    first = jnp.where(odd, sine, cosine)
    second = jnp.where(odd, cosine, sine)
    first = jnp.where((quarter == 1) | (quarter == 2), -first, first)
    second = jnp.where(quarter >= 2, -second, second)
    return first, second


def turn_kernel(psi_ref, angle_ref, out_ref):
    cosine, sine = cos_sin(angle_ref[...])
    for g in range(psi_ref.shape[1]):
        band = slice(g * LANE_ROWS, (g + 1) * LANE_ROWS)
        turn_re, turn_im = cosine[:, band], sine[:, band]
        for l in range(psi_ref.shape[0]):
            real_part, imag_part = psi_ref[l, g, 0], psi_ref[l, g, 1]
            out_ref[l, 0, :, band, :] = real_part * turn_re + imag_part * turn_im
            out_ref[l, 1, :, band, :] = imag_part * turn_re - real_part * turn_im


def turn(evolved, angle):
    layers, groups, _, planes, _, nz = evolved.shape
    ny = groups * LANE_ROWS
    bx = min(4, planes)
    field_block = pl.BlockSpec((bx, ny, nz), lambda i: (i, 0, 0))
    return pl.pallas_call(
        turn_kernel,
        grid=(planes // bx,),
        in_specs=[
            pl.BlockSpec((layers, groups, 2, bx, LANE_ROWS, nz), lambda i: (0, 0, 0, i, 0, 0)),
            field_block,
        ],
        out_specs=pl.BlockSpec((layers, 2, bx, ny, nz), lambda i: (0, 0, i, 0, 0)),
        out_shape=jax.ShapeDtypeStruct((layers, 2, planes, ny, nz), jnp.float32),
        compiler_params=pltpu.CompilerParams(vmem_limit_bytes=VMEM_LIMIT),
    )(evolved, angle)


def rotate_kernel(layers, *refs):
    cos_ref, sin_ref = refs[layers], refs[layers + 1]
    out_ref = refs[layers + 2]
    grid_count, _, _, vy, _ = refs[0].shape
    for g in range(grid_count):
        band = slice(g * vy, (g + 1) * vy)
        cosine = cos_ref[:, band, :]
        sine = sin_ref[:, band, :]
        for l in range(layers):
            real_part = refs[l][g, 0]
            imag_part = refs[l][g, 1]
            out_ref[l, 0, :, band, :] = real_part * cosine + imag_part * sine
            out_ref[l, 1, :, band, :] = imag_part * cosine - real_part * sine


def rotate(returned, cosine, sine):
    layers = len(returned)
    grid_count, _, planes, vy, nz = returned[0].shape
    ny = grid_count * vy
    bx = min(4, planes)
    field_block = pl.BlockSpec((bx, ny, nz), lambda i: (i, 0, 0))
    return pl.pallas_call(
        partial(rotate_kernel, layers),
        grid=(planes // bx,),
        in_specs=[pl.BlockSpec((grid_count, 2, bx, vy, nz), lambda i: (0, 0, i, 0, 0))] * layers
        + [field_block, field_block],
        out_specs=pl.BlockSpec((layers, 2, bx, ny, nz), lambda i: (0, 0, i, 0, 0)),
        out_shape=jax.ShapeDtypeStruct((layers, 2, planes, ny, nz), jnp.float32),
        compiler_params=pltpu.CompilerParams(vmem_limit_bytes=VMEM_LIMIT),
    )(*returned, cosine, sine)


def table_of(matrix):
    return (np.asarray(matrix.real, np.float32), np.asarray(matrix.imag, np.float32))


def apply_along(values, table, axis):
    contracted = jnp.tensordot(values, table, axes=([axis], [0]), precision=HIGHEST)
    return jnp.moveaxis(contracted, -1, axis)


def complex_along(real_part, imag_part, matrix, axis):
    table_re, table_im = table_of(matrix)
    new_re = apply_along(real_part, table_re, axis) - apply_along(imag_part, table_im, axis)
    new_im = apply_along(real_part, table_im, axis) + apply_along(imag_part, table_re, axis)
    return (new_re, new_im)


def coulomb_kernel(squares_x, squares_y, squares_z):
    total = squares_x[:, None, None] + squares_y[None, :, None] + squares_z[None, None, :]
    anchor = total <= 0.0
    return jnp.where(anchor, 0.0, HARTREE_SCALE / jnp.where(anchor, 1.0, total))


def poisson_shared(density):
    width_x, _, count_z = density.shape
    span_count = lax.axis_size("grid") * lax.axis_size("orb")
    block_x = width_x // span_count
    forward_z = table_of(fourier(count_z, -1))
    real_part, imag_part = (apply_along(density, forward_z[0], 2), apply_along(density, forward_z[1], 2))
    real_part, imag_part = complex_along(real_part, imag_part, fourier(width_x, -1), 0)
    spread = lax.all_to_all(
        jnp.stack([real_part, imag_part], 0),
        ("grid", "orb"),
        split_axis=1,
        concat_axis=2,
        tiled=True,
    )
    count_y = spread.shape[2]
    real_part, imag_part = complex_along(spread[0], spread[1], fourier(count_y, -1), 1)
    start_x = lax.axis_index(("grid", "orb")) * block_x
    squares_x = lax.dynamic_slice_in_dim(
        jnp.asarray(wave_squared(width_x), jnp.float32), start_x, block_x, 0
    )
    kernel = coulomb_kernel(
        squares_x,
        np.asarray(wave_squared(count_y), np.float32),
        np.asarray(wave_squared(count_z), np.float32),
    )
    real_part, imag_part = complex_along(
        real_part * kernel, imag_part * kernel, fourier(count_y, 1) / count_y, 1
    )
    back = lax.all_to_all(
        jnp.stack([real_part, imag_part], 0),
        ("grid", "orb"),
        split_axis=2,
        concat_axis=1,
        tiled=True,
    )
    real_part, imag_part = complex_along(back[0], back[1], fourier(width_x, 1) / width_x, 0)
    inverse_z = table_of(fourier(count_z, 1) / count_z)
    return apply_along(real_part, inverse_z[0], 2) - apply_along(imag_part, inverse_z[1], 2)


def body(orbitals, v_local, occupations):
    layers, _, planes, count_y, count_z = orbitals.shape
    grid_count = lax.axis_size("grid")
    orb_count = lax.axis_size("orb")
    width_x = planes * grid_count
    share_y = count_y // (grid_count * orb_count)
    wz = jnp.asarray(split_const(right_block(kinetic_matrix(count_z))))
    wy = jnp.asarray(split_const(left_block(kinetic_matrix(count_y))))
    order = np.arange(2 * width_x).reshape(2, grid_count, planes).transpose(1, 0, 2).reshape(-1)
    wx = jnp.asarray(split_const(left_block(kinetic_matrix(width_x))[order][:, order]))
    weights = lax.dynamic_slice_in_dim(occupations, lax.axis_index("orb") * layers, layers, 0)
    if (
        grid_count == 4
        and orb_count == 4
        and layers >= 4
        and planes % 8 == 0
        and count_y % (8 * LANE_ROWS) == 0
        and count_z % 128 == 0
    ):
        evolved, angle = evolve(orbitals, v_local, weights, wz, wy)
        return turn(evolved, angle)

    exchange = partial(lax.all_to_all, axis_name="grid", split_axis=0, concat_axis=0, tiled=True)

    received = [
        exchange(kinetic_local(orbitals, layer, grid_count, wz, wy)) for layer in range(layers)
    ]
    density = None
    returned = []
    for layer in range(layers):
        moved, density = kinetic_across(
            received[layer], weights[layer : layer + 1], density, wx
        )
        returned.append(exchange(moved))
    share = lax.psum_scatter(density, "orb", scatter_dimension=1, tiled=True)
    share, returned[0] = lax.optimization_barrier((share, returned[0]))
    hartree_lines = poisson_shared(share)
    rows_back = lax.all_to_all(hartree_lines, "grid", split_axis=0, concat_axis=1, tiled=True)
    gathered = lax.all_gather(rows_back, "orb", axis=0, tiled=False)
    hartree = gathered.reshape(orb_count, planes, grid_count, share_y, count_z)
    hartree = hartree.transpose(1, 2, 0, 3, 4).reshape(planes, count_y, count_z)
    angle = TIME_STEP * (v_local + hartree)
    return rotate(returned, jnp.cos(angle), jnp.sin(angle))


def solution(mesh):
    return jax.shard_map(
        body,
        mesh=mesh,
        in_specs=(
            P(("groups", "orb"), None, "grid", None, None),
            P(("groups", "grid"), None, None),
            P("groups"),
        ),
        out_specs=P(("groups", "orb"), None, "grid", None, None),
        check_vma=False,
    )
```

```python
from functools import partial
import math

import jax
import jax.numpy as jnp
import ml_dtypes
import numpy as np
from jax import lax
from jax.experimental import pallas as pl
from jax.experimental.pallas import tpu as pltpu
from jax.sharding import PartitionSpec as P

TIME_STEP = 0.05
KINETIC_RATE = 0.1
HARTREE_SCALE = math.pi
HIGHEST = lax.Precision.HIGHEST
VMEM_LIMIT = 50 * 1024 * 1024


def wave_squared(length):
    ids = np.arange(length)
    signed = np.where(ids < (length + 1) // 2, ids, ids - length)
    return (2.0 * np.pi * signed / length) ** 2


def fourier(length, sign):
    ids = np.arange(length)
    return np.exp(sign * 2j * np.pi * ((ids[:, None] * ids[None, :]) % length) / length)


def kinetic_matrix(length):
    phase = np.exp(-1j * KINETIC_RATE * wave_squared(length))
    return (fourier(length, 1) / length * phase[None, :]) @ fourier(length, -1)


def left_block(matrix):
    return np.block([[matrix.real, -matrix.imag], [matrix.imag, matrix.real]])


def right_block(matrix):
    return np.block([[matrix.real, matrix.imag], [-matrix.imag, matrix.real]])


def split_const(table):
    table = np.asarray(table, np.float32)
    high = table.astype(ml_dtypes.bfloat16)
    low = (table - high.astype(np.float32)).astype(ml_dtypes.bfloat16)
    return np.stack([high, low])


def split(values):
    high = values.astype(jnp.bfloat16)
    low = (values - high.astype(jnp.float32)).astype(jnp.bfloat16)
    return high, low


def dot(left, right):
    return jnp.dot(left, right, preferred_element_type=jnp.float32)


def data_by_table(values, table):
    high, low = split(values)
    return dot(high, table[0]) + dot(high, table[1]) + dot(low, table[0])


def table_by_data(table, values):
    high, low = split(values)
    return dot(table[0], high) + dot(table[1], high) + dot(table[0], low)


def local_kernel(psi_ref, wz_ref, wy_ref, out_ref):
    _, _, bx, ny, nz = psi_ref.shape
    grid_count, _, _, vy, _ = out_ref.shape
    real_part = psi_ref[0, 0].reshape(bx * ny, nz)
    imag_part = psi_ref[0, 1].reshape(bx * ny, nz)
    turned = data_by_table(jnp.concatenate([real_part, imag_part], 1), wz_ref)
    columns = [
        jnp.concatenate(
            [turned[p * ny : (p + 1) * ny, :nz], turned[p * ny : (p + 1) * ny, nz:]], 0
        )
        for p in range(bx)
    ]
    rows = table_by_data(wy_ref, jnp.concatenate(columns, 1))
    for g in range(grid_count):
        for c in range(2):
            start = c * ny + g * vy
            for p in range(bx):
                out_ref[g, c, p] = rows[start : start + vy, p * nz : (p + 1) * nz]


def kinetic_local(orbitals, layer, grid_count, wz, wy):
    _, _, planes, ny, nz = orbitals.shape
    bx = min(4, planes)
    vy = ny // grid_count
    return pl.pallas_call(
        local_kernel,
        grid=(planes // bx,),
        in_specs=[
            pl.BlockSpec((1, 2, bx, ny, nz), lambda i: (layer, 0, i, 0, 0)),
            pl.BlockSpec(wz.shape, lambda i: (0, 0, 0)),
            pl.BlockSpec(wy.shape, lambda i: (0, 0, 0)),
        ],
        out_specs=pl.BlockSpec((grid_count, 2, bx, vy, nz), lambda i: (0, 0, i, 0, 0)),
        out_shape=jax.ShapeDtypeStruct((grid_count, 2, planes, vy, nz), jnp.float32),
        compiler_params=pltpu.CompilerParams(vmem_limit_bytes=VMEM_LIMIT),
        cost_estimate=pl.CostEstimate(
            flops=3 * 8 * planes * ny * nz * (ny + nz),
            bytes_accessed=16 * planes * ny * nz,
            transcendentals=0,
        ),
    )(orbitals, wz, wy)


def across_kernel(planes, first, weight_ref, psi_ref, wx_ref, *refs):
    if first:
        out_ref, density_ref = refs
    else:
        earlier_ref, out_ref, density_ref = refs
    depth, by, nz = psi_ref.shape
    columns = jnp.concatenate([psi_ref[:, j, :] for j in range(by)], 1)
    moved = table_by_data(wx_ref, columns)
    squares = moved * moved
    weight = weight_ref[0]
    for j in range(by):
        out_ref[:, j, :] = moved[:, j * nz : (j + 1) * nz]
    for h in range(depth // (2 * planes)):
        low = 2 * h * planes
        term = weight * (squares[low : low + planes] + squares[low + planes : low + 2 * planes])
        for j in range(by):
            value = term[:, j * nz : (j + 1) * nz]
            if not first:
                value = value + earlier_ref[h * planes : (h + 1) * planes, j, :]
            density_ref[h * planes : (h + 1) * planes, j, :] = value


def kinetic_across(received, weight, density, wx):
    grid_count, _, planes, vy, nz = received.shape
    depth = grid_count * 2 * planes
    by = min(8, vy)
    first = density is None
    block = pl.BlockSpec((depth, by, nz), lambda i: (0, i, 0))
    density_block = pl.BlockSpec((depth // 2, by, nz), lambda i: (0, i, 0))
    in_specs = [
        pl.BlockSpec(memory_space=pltpu.SMEM),
        block,
        pl.BlockSpec(wx.shape, lambda i: (0, 0, 0)),
    ]
    operands = [weight, received.reshape(depth, vy, nz), wx]
    if not first:
        in_specs.append(density_block)
        operands.append(density)
    moved, density = pl.pallas_call(
        partial(across_kernel, planes, first),
        grid=(vy // by,),
        in_specs=in_specs,
        out_specs=[block, density_block],
        out_shape=[
            jax.ShapeDtypeStruct((depth, vy, nz), jnp.float32),
            jax.ShapeDtypeStruct((depth // 2, vy, nz), jnp.float32),
        ],
        compiler_params=pltpu.CompilerParams(vmem_limit_bytes=VMEM_LIMIT),
        cost_estimate=pl.CostEstimate(
            flops=3 * 2 * depth * depth * vy * nz,
            bytes_accessed=12 * depth * vy * nz,
            transcendentals=0,
        ),
    )(*operands)
    return moved.reshape(grid_count, 2, planes, vy, nz), density


LANE_ROWS = 8
MESH = pl.DeviceIdType.MESH
EPS = float(np.finfo(np.float32).eps)


def far_factors(block):
    block = block.astype(np.clongdouble)
    norm2 = np.sum(np.abs(block) ** 2)
    residual = block.copy()
    rank = 0
    basis = []
    for _ in range(block.shape[1]):
        sizes = np.sum(np.abs(residual) ** 2, axis=1)
        if np.sum(sizes) <= (EPS * EPS) * 1e-3 * norm2:
            break
        row = residual[int(np.argmax(sizes))].conj()
        for other in basis:
            row = row - other * np.sum(other.conj() * row)
        row = row / np.sqrt(np.sum(np.abs(row) ** 2))
        basis.append(row)
        residual = residual - np.sum(residual * row[None, :], axis=1)[:, None] * row.conj()[None, :]
    gram = np.matmul(block.conj().T, block)
    for _ in range(8):
        basis = [np.sum(gram * vector[None, :], axis=1) for vector in basis]
        clean = []
        for row in basis:
            for _ in range(2):
                for other in clean:
                    row = row - other * np.sum(other.conj() * row)
            clean.append(row / np.sqrt(np.sum(np.abs(row) ** 2)))
        basis = clean
    for rank in range(1, len(basis) + 1):
        right = np.stack(basis[:rank], 1)
        left = np.matmul(block, right)
        rest = block - np.matmul(left, right.conj().T)
        if np.linalg.norm(rest.astype(np.complex128), 2) <= EPS:
            break
    return left.astype(np.complex128), right.astype(np.complex128)


def real_form(matrix):
    return np.block([[matrix.real, -matrix.imag], [matrix.imag, matrix.real]])


def stacked_table(table):
    high, low = split_const(table).astype(np.float32)
    return np.block([[high, high], [low, np.zeros_like(low)]]).astype(ml_dtypes.bfloat16)


def evolve_tables(width_x, planes):
    matrix = kinetic_matrix(width_x)
    half = 2 * planes
    left, right = far_factors(matrix[half:, :half])
    rank = -(-left.shape[1] // 2) * 2
    pad = rank - left.shape[1]
    left = np.pad(left, ((0, 0), (0, pad)))
    right = np.pad(right, ((0, 0), (0, pad)))
    near = matrix[:planes, :planes]
    sides = []
    for core in range(2):
        mine = slice(core * planes, (core + 1) * planes)
        theirs = slice((1 - core) * planes, (2 - core) * planes)
        sides.append(
            (left[mine], right[mine], far_factors(matrix[theirs, mine]), far_factors(matrix[mine, theirs]))
        )
    core_rank = max(s[2][0].shape[1] for s in sides)
    core_rank = -(-core_rank // 4) * 4
    widen = lambda m: np.pad(m, ((0, 0), (0, core_rank - m.shape[1])))
    far = -(-2 * rank // 8) * 8
    gather, spread = [], []
    for mine_left, mine_right, (_, give), (take, _) in sides:
        rows = real_form(mine_right.conj().T)
        rows = np.concatenate([rows, np.zeros((far - rows.shape[0], rows.shape[1]))], 0)
        core_rows = real_form(widen(give).conj().T)
        gather.append(stacked_table(np.concatenate([rows, core_rows], 0)))
        far_columns = real_form(mine_left)
        far_columns = np.pad(far_columns, ((0, 0), (0, far - far_columns.shape[1])))
        spread.append(
            stacked_table(np.concatenate([real_form(near), real_form(widen(take)), far_columns], 1))
        )
    return np.stack(gather), np.stack(spread), 2 * rank, far, 2 * core_rank


def stack_split(values):
    high, low = split(values)
    return jnp.concatenate([high, low], 0)


def split_three(values):
    high = values.astype(jnp.bfloat16)
    rest = values - high.astype(jnp.float32)
    middle = rest.astype(jnp.bfloat16)
    low = (rest - middle.astype(jnp.float32)).astype(jnp.bfloat16)
    return [high, middle, low]


def six_table(table):
    parts, rest = [], np.asarray(table, np.float32)
    for _ in range(3):
        parts.append(rest.astype(ml_dtypes.bfloat16).astype(np.float32))
        rest = rest - parts[-1]
    high, middle, low = parts
    return np.concatenate([high, high, high, middle, middle, low], 1).astype(ml_dtypes.bfloat16)


def six_parts(values):
    high, middle, low = split_three(values)
    return [high, middle, low, high, middle, high]


def exact_left(table_ref, values):
    return dot(table_ref[...], jnp.concatenate(six_parts(values), 0))


def exact_right(values, table_ref):
    parts = six_parts(values)
    width = values.shape[1]
    total = None
    for pair in range(3):
        data = jnp.concatenate(parts[2 * pair : 2 * pair + 2], 1)
        term = dot(data, table_ref[2 * pair * width : 2 * (pair + 1) * width, :])
        total = term if total is None else total + term
    return total


def real_basis(length):
    ids = np.arange(length)
    angle = 2.0 * np.pi * ((ids[:, None] * ids[None, :]) % length) / length
    table = np.where(ids[None, :] <= length // 2, np.cos(angle), np.sin(angle))
    single = (ids == 0) | (2 * ids == length)
    return table * np.where(single, 1.0, math.sqrt(2.0))[None, :] / math.sqrt(length)


def rows_at(ref, row):
    return ref[pl.ds(row, ref.shape[0] // LANE_ROWS, stride=LANE_ROWS), :]


def put_rows(ref, row, values):
    ref[pl.ds(row, ref.shape[0] // LANE_ROWS, stride=LANE_ROWS), :] = values


def tile_of(index):
    return pl.ds(pl.multiple_of(index * LANE_ROWS, LANE_ROWS), LANE_ROWS)


def evolve_kernel(
    layers, far_rows, far, near_rows, lag,
    weight_ref, wave_ref, psi_ref, local_ref, wz_ref, wy_ref, gather_ref, spread_ref,
    qz_ref, qzt_ref, qy_ref, qyt_ref, qx_ref, qxt_ref, plane_wave_ref,
    out_ref, angle_ref,
    stage, phi, give_far, give_near, got_far, got_near, far_field, result, density,
    outer_sum, middle_sum, total, spectrum, lines, returned, local,
    in_sem, out_sem, p_send, p_recv, q_send, q_recv, y_send, y_recv, f_send, f_recv,
    a_send, a_recv, m_send, m_recv, t_send, t_recv, l_send, l_recv, b_send, b_recv, d_send, d_recv, v_sem,
):
    _, _, planes, ny, nz = psi_ref.shape
    groups = ny // LANE_ROWS
    tiles = groups // 2
    units = layers * tiles
    bx = stage.shape[2]
    per_layer = planes // bx
    steps = layers * per_layer
    paired = (layers - 3) * tiles
    place = lax.axis_index("grid")
    core = lax.rem(place, 2)
    sibling = place + 1 - 2 * core
    across = lax.rem(place + 2, 4)
    depth = lax.axis_index("orb")
    outer = (depth == 0) | (depth == 3)
    inner = (depth == 1) | (depth == 2)
    toward = 1 + depth // 3
    outward = jnp.where(depth == 1, 0, 3)
    middle = jnp.where(depth == 1, 2, 1)

    def where_is(unit):
        late = unit - paired
        layer = jnp.where(late < 0, unit // tiles, layers - 3 + lax.rem(jnp.maximum(late, 0), 3))
        tile = jnp.where(late < 0, lax.rem(unit, tiles), jnp.maximum(late, 0) // 3)
        return layer, tile

    def remote(source, target, send_sem, recv_sem, device):
        return pltpu.make_async_remote_copy(
            src_ref=source, dst_ref=target, send_sem=send_sem, recv_sem=recv_sem,
            device_id=device, device_id_type=MESH,
        )

    def far_copy(unit):
        return remote(
            give_far.at[lax.rem(unit, 4), 1 - core], got_far.at[unit],
            p_send.at[unit], p_recv.at[unit], {"grid": sibling},
        )

    def near_copy(unit):
        return remote(
            give_near.at[lax.rem(unit, 4)], got_near.at[unit],
            q_send.at[unit], q_recv.at[unit], {"grid": sibling},
        )

    def across_copy(unit):
        return remote(
            got_far.at[unit], far_field.at[unit, core, pl.ds(0, far_rows * LANE_ROWS)],
            y_send.at[unit], y_recv.at[unit], {"grid": across},
        )

    def share_copy(unit):
        held = far_field.at[unit, core, pl.ds(0, far_rows * LANE_ROWS)]
        return remote(held, held, f_send.at[unit], f_recv.at[unit], {"grid": sibling})

    piece = planes * LANE_ROWS // 2

    def piece_of(ref, g, p):
        return ref.at[g, pl.ds(p * piece, piece)]

    def outer_copy(g, p):
        return remote(
            piece_of(density, g, p), piece_of(outer_sum, g, p), a_send.at[g, p], a_recv.at[g, p], {"orb": toward}
        )

    def middle_copy(g, p):
        return remote(
            piece_of(density, g, p), piece_of(middle_sum, g, p), m_send.at[g, p], m_recv.at[g, p], {"orb": middle}
        )

    def total_copy(g, p):
        held = piece_of(total, g, p)
        return remote(held, held, t_send.at[g, p], t_recv.at[g, p], {"orb": outward})

    def pieces(tile):
        return [(2 * tile + g, p) for g in range(2) for p in range(2)]

    def load_copy(step):
        layer, part = step // per_layer, lax.rem(step, per_layer)
        slot = lax.rem(step, 3)
        return pltpu.make_async_copy(
            psi_ref.at[layer, :, pl.ds(part * bx, bx)], stage.at[slot], in_sem.at[slot]
        )

    def result_copy(unit, half):
        layer, tile = where_is(unit)
        slot = lax.rem(unit, 3)
        return pltpu.make_async_copy(
            result.at[slot, half],
            out_ref.at[layer, 2 * tile + half],
            out_sem.at[slot, half],
        )

    load_copy(0).start()
    load_copy(1).start()
    local_copy = pltpu.make_async_copy(local_ref, local, v_sem)
    local_copy.start()
    if far > far_rows:
        far_field[:, :, far_rows * LANE_ROWS :] = jnp.zeros((units, 2, (far - far_rows) * LANE_ROWS, nz), jnp.float32)
    density[...] = jnp.zeros_like(density)
    barrier = pltpu.get_barrier_semaphore()
    for k in range(1, 4):
        pl.semaphore_signal(barrier, inc=1, device_id={"grid": lax.rem(place + k, 4)}, device_id_type=MESH)

    @pl.when(outer)
    def _():
        pl.semaphore_signal(barrier, inc=1, device_id={"orb": toward}, device_id_type=MESH)

    @pl.when(inner)
    def _():
        pl.semaphore_signal(barrier, inc=1, device_id={"orb": outward}, device_id_type=MESH)
        pl.semaphore_signal(barrier, inc=1, device_id={"orb": middle}, device_id_type=MESH)

    def plane_step(step, carry):
        @pl.when(step + 2 < steps)
        def _():
            load_copy(step + 2).start()

        load_copy(step).wait()
        layer, part = step // per_layer, lax.rem(step, per_layer)
        slot = lax.rem(step, 3)
        real_part = stage[slot, 0].reshape(bx * ny, nz)
        imag_part = stage[slot, 1].reshape(bx * ny, nz)
        turned = data_by_table(jnp.concatenate([real_part, imag_part], 1), wz_ref)
        columns = [
            jnp.concatenate([turned[p * ny : (p + 1) * ny, :nz], turned[p * ny : (p + 1) * ny, nz:]], 0)
            for p in range(bx)
        ]
        rows = table_by_data(wy_ref, jnp.concatenate(columns, 1))
        for c in range(2):
            for p in range(bx):
                block = rows[c * ny : (c + 1) * ny, p * nz : (p + 1) * nz]
                phi[layer, :, tile_of(c * planes + part * bx + p), :] = block.reshape(groups, LANE_ROWS, nz)
        return carry

    def gather_step(unit):
        layer, tile = where_is(unit)
        slot = lax.rem(unit, 4)

        @pl.when(unit >= 4)
        def _():
            far_copy(unit - 4).wait_send()
            near_copy(unit - 4).wait_send()

        for half in range(2):
            for part in range(2):
                ids = range(4 * part, 4 * part + 4)
                source = phi.at[layer, 2 * tile + half]
                data = jnp.concatenate([rows_at(source, i) for i in ids], 1)
                both = dot(gather_ref[core], stack_split(data))
                joined = both[: far + near_rows] + both[far + near_rows :]
                for k, i in enumerate(ids):
                    block = joined[:, k * nz : (k + 1) * nz]
                    put_rows(give_far.at[slot, half], i, block[:far_rows])
                    put_rows(give_near.at[slot, half], i, block[far:])

    def sum_step(unit):
        far_copy(unit).wait_recv()
        got_far[unit] = got_far[unit] + give_far[lax.rem(unit, 4), core]

    def spread_step(unit):
        layer, tile = where_is(unit)
        slot = lax.rem(unit, 3)
        near_copy(unit).wait_recv()
        share_copy(unit).wait_recv()

        @pl.when(unit >= 3)
        def _():
            result_copy(unit - 3, 0).wait()
            result_copy(unit - 3, 1).wait()

        weight = weight_ref[depth * layers + layer]
        for half in range(2):
            for part in range(2):
                ids = range(4 * part, 4 * part + 4)
                data = jnp.concatenate(
                    [
                        jnp.concatenate(
                            [
                                rows_at(phi.at[layer, 2 * tile + half], i),
                                rows_at(got_near.at[unit, half], i),
                                rows_at(far_field.at[unit, half], i),
                            ],
                            0,
                        )
                        for i in ids
                    ],
                    1,
                )
                both = dot(spread_ref[core], stack_split(data))
                moved = both[: 2 * planes] + both[2 * planes :]
                squares = moved * moved
                term = weight * (squares[:planes] + squares[planes:])
                for k, i in enumerate(ids):
                    put_rows(result.at[slot, half], i, moved[:, k * nz : (k + 1) * nz])
                    summed = density.at[2 * tile + half]
                    put_rows(summed, i, rows_at(summed, i) + term[:, k * nz : (k + 1) * nz])

    def send(unit):
        far_copy(unit).start()
        near_copy(unit).start()

    def forward(unit):
        across_copy(unit).wait_recv()
        share_copy(unit).start()

    def write(unit):
        result_copy(unit, 0).start()
        result_copy(unit, 1).start()

    def start_outer(tile):
        for g, p in pieces(tile):
            outer_copy(g, p).start()

    def add_outer(tile):
        held = None
        for g, p in pieces(tile):
            outer_copy(g, p).wait_recv()
            rows = pl.ds(p * piece, piece)
            density[g, rows] = density[g, rows] + outer_sum[g, rows]
            if held is not None:
                middle_copy(*held).start()
            held = (g, p)

    def start_middle(tile):
        middle_copy(2 * tile + 1, 1).start()

    def add_middle(tile):
        held = None
        for g, p in pieces(tile):
            middle_copy(g, p).wait_recv()
            rows = pl.ds(p * piece, piece)
            total[g, rows] = density[g, rows] + middle_sum[g, rows]
            if held is not None:
                total_copy(*held).start()
            held = (g, p)

    def start_total(tile):
        total_copy(2 * tile + 1, 1).start()
        for g in range(2):
            flatten(2 * tile + g)

    def flatten(g):
        outer_sum[g] = exact_right(total[g], qz_ref)

    def receive(tile):
        for g in range(2):
            for p in range(2):
                total_copy(2 * tile + g, p).wait_recv()
            flatten(2 * tile + g)

    def prepared(t):
        late = jnp.maximum(t - 2, 0)
        return jnp.minimum(per_layer + (late * (layers - 1) * per_layer) // (paired - 2), steps)

    first_forward = 3 + lag
    first_spread = first_forward + 2
    ready = first_spread + 1
    last = ready + 15

    def tick(t, carry):
        def stage_at(start, action):
            unit = t - start

            @pl.when((unit >= 0) & (unit < units))
            def _():
                action(unit)

        def reduce_at(start, who, action):
            late = t - start - paired

            @pl.when((late >= 0) & (late < 3 * tiles) & (lax.rem(late + 3 * units, 3) == 2) & who)
            def _():
                action(late // 3)

        stage_at(1, send)
        stage_at(3, lambda unit: across_copy(unit).start())
        stage_at(ready, write)
        reduce_at(ready, outer, start_outer)
        reduce_at(ready + 4, inner, add_outer)
        reduce_at(ready + 5, inner, start_middle)
        reduce_at(ready + 9, inner, add_middle)
        reduce_at(ready + 10, inner, start_total)
        reduce_at(ready + 15, outer, receive)
        lax.fori_loop(prepared(t), prepared(t + 1), plane_step, 0)
        stage_at(2, sum_step)
        stage_at(0, gather_step)
        stage_at(first_forward, forward)
        stage_at(first_spread, spread_step)
        return carry

    lax.fori_loop(0, per_layer, plane_step, 0)

    @pl.when(outer)
    def _():
        pl.semaphore_wait(barrier, 4)

    @pl.when(inner)
    def _():
        pl.semaphore_wait(barrier, 5)

    lax.fori_loop(0, last + units, tick, 0)

    local_copy.wait()

    four = 4

    def spectrum_step(part, carry):
        ids = [part * four + p for p in range(four)]
        moved = exact_left(
            qyt_ref, jnp.concatenate([outer_sum[:, tile_of(x), :].reshape(ny, nz) for x in ids], 1)
        )
        for p, x in enumerate(ids):
            spectrum[:, tile_of(x), :] = moved[:, p * nz : (p + 1) * nz].reshape(groups, LANE_ROWS, nz)
        return carry

    lax.fori_loop(0, planes // four, spectrum_step, 0)
    share = groups // 8
    span = planes * LANE_ROWS
    mine = lax.rem(depth, 2) * (groups // 2)
    other = groups // 2 - mine
    partner = depth + 1 - 2 * lax.rem(depth, 2)

    def lines_of(device):
        return pl.ds(pl.multiple_of(device * span, span), span)

    def line_copy(g, k):
        peer = lax.rem(place + k, 4)
        return remote(
            spectrum.at[mine + peer * share + g], lines.at[g, lines_of(place)],
            l_send.at[g, k - 1], l_recv.at[g, k - 1], {"grid": peer},
        )

    def back_copy(g, k):
        peer = lax.rem(place + k, 4)
        return remote(
            lines.at[g, lines_of(peer)], returned.at[mine + place * share + g],
            b_send.at[g, k - 1], b_recv.at[g, k - 1], {"grid": peer},
        )

    def pair_copy(row):
        return remote(
            returned.at[row], returned.at[row],
            d_send.at[row], d_recv.at[row], {"orb": partner},
        )

    for g in range(share):
        for k in (2, 3, 1):
            line_copy(g, k).start()
        lines[g, lines_of(place)] = spectrum[mine + place * share + g]

    for g in range(share):
        for k in (1, 2, 3):
            line_copy(g, k).wait_recv()
        for part in range(2):
            ids = range(4 * part, 4 * part + 4)
            data = jnp.concatenate([rows_at(lines.at[g], i) for i in ids], 1)
            modes = exact_left(qxt_ref, data)
            scaled = []
            for k, i in enumerate(ids):
                waves = plane_wave_ref[...] + wave_ref[(mine + place * share + g) * LANE_ROWS + i]
                anchor = waves <= 0.0
                kernel = jnp.where(anchor, 0.0, HARTREE_SCALE / jnp.where(anchor, 1.0, waves))
                scaled.append(modes[:, k * nz : (k + 1) * nz] * kernel)
            moved = exact_left(qx_ref, jnp.concatenate(scaled, 1))
            for k, i in enumerate(ids):
                put_rows(lines.at[g], i, moved[:, k * nz : (k + 1) * nz])
        row = mine + place * share + g
        returned[row] = lines[g, lines_of(place)]
        for k in (2, 1, 3):
            back_copy(g, k).start()
        pair_copy(row).start()
    for g in range(share):
        for k in (1, 2, 3):
            line_copy(g, k).wait_send()

    def straighten(row):
        spectrum[row] = exact_right(returned[row], qzt_ref)

    for g in range(share):
        straighten(mine + place * share + g)
    for g in range(share):
        for k in (3, 1, 2):
            row = mine + lax.rem(place + 4 - k, 4) * share + g
            back_copy(g, k).wait_recv()
            pair_copy(row).start()
            straighten(row)

    def finish(unit, carry):
        across_copy(unit).wait_send()
        share_copy(unit).wait_send()

        @pl.when(unit >= units - 4)
        def _():
            far_copy(unit).wait_send()
            near_copy(unit).wait_send()

        @pl.when(unit >= units - 3)
        def _():
            result_copy(unit, 0).wait()
            result_copy(unit, 1).wait()

        return carry

    lax.fori_loop(0, units, finish, 0)

    @pl.when(outer)
    def _():
        for g in range(groups):
            for p in range(2):
                outer_copy(g, p).wait_send()

    @pl.when(inner)
    def _():
        for g in range(groups):
            for p in range(2):
                middle_copy(g, p).wait_send()
                total_copy(g, p).wait_send()

    for k in (0, 3, 1, 2):
        for g in range(share):
            row = other + lax.rem(place + 4 - k, 4) * share + g
            pair_copy(row).wait_recv()
            straighten(row)

    def potential_step(part, carry):
        ids = [part * four + p for p in range(four)]
        moved = exact_left(
            qy_ref, jnp.concatenate([spectrum[:, tile_of(x), :].reshape(ny, nz) for x in ids], 1)
        )
        for p, x in enumerate(ids):
            angle_ref[x] = TIME_STEP * (local[x] + moved[:, p * nz : (p + 1) * nz])
        return carry

    lax.fori_loop(0, planes // four, potential_step, 0)
    for g in range(share):
        for k in (1, 2, 3):
            back_copy(g, k).wait_send()

    def settle(row, carry):
        pair_copy(mine + row).wait_send()
        return carry

    lax.fori_loop(0, groups // 2, settle, 0)


def evolve(orbitals, v_local, occupations, wz, wy):
    layers, _, planes, ny, nz = orbitals.shape
    width_x = 4 * planes
    gather, spread, far_rows, far, near_rows = evolve_tables(width_x, planes)
    groups = ny // LANE_ROWS
    tiles = groups // 2
    units = layers * tiles
    f32 = jnp.float32
    squares = [wave_squared(n).astype(np.float32) for n in (width_x, ny, nz)]
    plane_wave = squares[0][:, None] + squares[2][None, :]
    basis = [real_basis(n) for n in (width_x, ny, nz)]
    tables = [
        six_table(basis[2].T).T, six_table(basis[2]).T, six_table(basis[1]), six_table(basis[1].T),
        six_table(basis[0]), six_table(basis[0].T), plane_wave,
    ]
    vmem = pl.BlockSpec(memory_space=pltpu.VMEM)
    smem = pl.BlockSpec(memory_space=pltpu.SMEM)
    anywhere = pl.BlockSpec(memory_space=pl.ANY)
    dma = pltpu.SemaphoreType.DMA
    field = pltpu.VMEM((groups, planes * LANE_ROWS, nz), f32)
    evolved, angle = pl.pallas_call(
        partial(evolve_kernel, layers, far_rows, far, near_rows, 3),
        in_specs=[smem, smem, anywhere, anywhere] + [vmem] * 11,
        out_specs=[anywhere, vmem],
        out_shape=[
            jax.ShapeDtypeStruct((layers, groups, 2 * planes * LANE_ROWS, nz), f32),
            jax.ShapeDtypeStruct((planes, ny, nz), f32),
        ],
        scratch_shapes=[
            pltpu.VMEM((3, 2, 8, ny, nz), f32),
            pltpu.VMEM((layers, groups, 2 * planes * LANE_ROWS, nz), f32),
            pltpu.VMEM((4, 2, far_rows * LANE_ROWS, nz), f32),
            pltpu.VMEM((4, 2, near_rows * LANE_ROWS, nz), f32),
            pltpu.VMEM((units, far_rows * LANE_ROWS, nz), f32),
            pltpu.VMEM((units, 2, near_rows * LANE_ROWS, nz), f32),
            pltpu.VMEM((units, 2, far * LANE_ROWS, nz), f32),
            pltpu.VMEM((3, 2, 2 * planes * LANE_ROWS, nz), f32),
            field, field, field, field, field,
            pltpu.VMEM((groups // 8, width_x * LANE_ROWS, nz), f32),
            field,
            pltpu.VMEM((planes, ny, nz), f32),
            dma((3,)),
            dma((3, 2)),
        ]
        + [dma((units,))] * 8
        + [dma((groups, 2))] * 6
        + [dma((groups // 8, 3))] * 4
        + [dma((groups,))] * 2
        + [pltpu.SemaphoreType.DMA],
        compiler_params=pltpu.CompilerParams(
            vmem_limit_bytes=63 * 1024 * 1024, collective_id=0, has_side_effects=True
        ),
        cost_estimate=pl.CostEstimate(
            flops=40 * layers * planes * ny * nz * (ny + nz), bytes_accessed=16 * layers * planes * ny * nz, transcendentals=0
        ),
    )(occupations, jnp.asarray(squares[1]), orbitals, v_local, wz, wy, *map(jnp.asarray, [gather, spread] + tables))
    return evolved.reshape(layers, groups, 2, planes, LANE_ROWS, nz), angle


def cos_sin(angle):
    turns = jnp.floor(angle * (2.0 / math.pi) + 0.5)
    rest = ((angle - turns * 1.5703125) - turns * 4.837512969970703125e-4) - turns * 7.549789954891882e-8
    square = rest * rest
    sine = ((-1.9515295891e-4 * square + 8.3321608736e-3) * square - 1.6666654611e-1) * square * rest + rest
    cosine = (
        (2.443315711809948e-5 * square - 1.388731625493765e-3) * square + 4.166664568298827e-2
    ) * square * square - 0.5 * square + 1.0
    quarter = turns.astype(jnp.int32) & 3
    odd = (quarter & 1) == 1
    first = jnp.where(odd, sine, cosine)
    second = jnp.where(odd, cosine, sine)
    first = jnp.where((quarter == 1) | (quarter == 2), -first, first)
    second = jnp.where(quarter >= 2, -second, second)
    return first, second


def turn_kernel(psi_ref, angle_ref, out_ref):
    cosine, sine = cos_sin(angle_ref[...])
    for g in range(psi_ref.shape[1]):
        band = slice(g * LANE_ROWS, (g + 1) * LANE_ROWS)
        turn_re, turn_im = cosine[:, band], sine[:, band]
        for l in range(psi_ref.shape[0]):
            real_part, imag_part = psi_ref[l, g, 0], psi_ref[l, g, 1]
            out_ref[l, 0, :, band, :] = real_part * turn_re + imag_part * turn_im
            out_ref[l, 1, :, band, :] = imag_part * turn_re - real_part * turn_im


def turn(evolved, angle):
    layers, groups, _, planes, _, nz = evolved.shape
    ny = groups * LANE_ROWS
    bx = min(8, planes)
    field_block = pl.BlockSpec((bx, ny, nz), lambda i: (i, 0, 0))
    return pl.pallas_call(
        turn_kernel,
        grid=(planes // bx,),
        in_specs=[
            pl.BlockSpec((layers, groups, 2, bx, LANE_ROWS, nz), lambda i: (0, 0, 0, i, 0, 0)),
            field_block,
        ],
        out_specs=pl.BlockSpec((layers, 2, bx, ny, nz), lambda i: (0, 0, i, 0, 0)),
        out_shape=jax.ShapeDtypeStruct((layers, 2, planes, ny, nz), jnp.float32),
        compiler_params=pltpu.CompilerParams(vmem_limit_bytes=63 * 1024 * 1024),
    )(evolved, angle)


def rotate_kernel(layers, *refs):
    cos_ref, sin_ref = refs[layers], refs[layers + 1]
    out_ref = refs[layers + 2]
    grid_count, _, _, vy, _ = refs[0].shape
    for g in range(grid_count):
        band = slice(g * vy, (g + 1) * vy)
        cosine = cos_ref[:, band, :]
        sine = sin_ref[:, band, :]
        for l in range(layers):
            real_part = refs[l][g, 0]
            imag_part = refs[l][g, 1]
            out_ref[l, 0, :, band, :] = real_part * cosine + imag_part * sine
            out_ref[l, 1, :, band, :] = imag_part * cosine - real_part * sine


def rotate(returned, cosine, sine):
    layers = len(returned)
    grid_count, _, planes, vy, nz = returned[0].shape
    ny = grid_count * vy
    bx = min(4, planes)
    field_block = pl.BlockSpec((bx, ny, nz), lambda i: (i, 0, 0))
    return pl.pallas_call(
        partial(rotate_kernel, layers),
        grid=(planes // bx,),
        in_specs=[pl.BlockSpec((grid_count, 2, bx, vy, nz), lambda i: (0, 0, i, 0, 0))] * layers
        + [field_block, field_block],
        out_specs=pl.BlockSpec((layers, 2, bx, ny, nz), lambda i: (0, 0, i, 0, 0)),
        out_shape=jax.ShapeDtypeStruct((layers, 2, planes, ny, nz), jnp.float32),
        compiler_params=pltpu.CompilerParams(vmem_limit_bytes=VMEM_LIMIT),
    )(*returned, cosine, sine)


def table_of(matrix):
    return (np.asarray(matrix.real, np.float32), np.asarray(matrix.imag, np.float32))


def apply_along(values, table, axis):
    contracted = jnp.tensordot(values, table, axes=([axis], [0]), precision=HIGHEST)
    return jnp.moveaxis(contracted, -1, axis)


def complex_along(real_part, imag_part, matrix, axis):
    table_re, table_im = table_of(matrix)
    new_re = apply_along(real_part, table_re, axis) - apply_along(imag_part, table_im, axis)
    new_im = apply_along(real_part, table_im, axis) + apply_along(imag_part, table_re, axis)
    return (new_re, new_im)


def coulomb_kernel(squares_x, squares_y, squares_z):
    total = squares_x[:, None, None] + squares_y[None, :, None] + squares_z[None, None, :]
    anchor = total <= 0.0
    return jnp.where(anchor, 0.0, HARTREE_SCALE / jnp.where(anchor, 1.0, total))


def poisson_shared(density):
    width_x, _, count_z = density.shape
    span_count = lax.axis_size("grid") * lax.axis_size("orb")
    block_x = width_x // span_count
    forward_z = table_of(fourier(count_z, -1))
    real_part, imag_part = (apply_along(density, forward_z[0], 2), apply_along(density, forward_z[1], 2))
    real_part, imag_part = complex_along(real_part, imag_part, fourier(width_x, -1), 0)
    spread = lax.all_to_all(
        jnp.stack([real_part, imag_part], 0),
        ("grid", "orb"),
        split_axis=1,
        concat_axis=2,
        tiled=True,
    )
    count_y = spread.shape[2]
    real_part, imag_part = complex_along(spread[0], spread[1], fourier(count_y, -1), 1)
    start_x = lax.axis_index(("grid", "orb")) * block_x
    squares_x = lax.dynamic_slice_in_dim(
        jnp.asarray(wave_squared(width_x), jnp.float32), start_x, block_x, 0
    )
    kernel = coulomb_kernel(
        squares_x,
        np.asarray(wave_squared(count_y), np.float32),
        np.asarray(wave_squared(count_z), np.float32),
    )
    real_part, imag_part = complex_along(
        real_part * kernel, imag_part * kernel, fourier(count_y, 1) / count_y, 1
    )
    back = lax.all_to_all(
        jnp.stack([real_part, imag_part], 0),
        ("grid", "orb"),
        split_axis=2,
        concat_axis=1,
        tiled=True,
    )
    real_part, imag_part = complex_along(back[0], back[1], fourier(width_x, 1) / width_x, 0)
    inverse_z = table_of(fourier(count_z, 1) / count_z)
    return apply_along(real_part, inverse_z[0], 2) - apply_along(imag_part, inverse_z[1], 2)


def body(orbitals, v_local, occupations):
    layers, _, planes, count_y, count_z = orbitals.shape
    grid_count = lax.axis_size("grid")
    orb_count = lax.axis_size("orb")
    width_x = planes * grid_count
    share_y = count_y // (grid_count * orb_count)
    wz = jnp.asarray(split_const(right_block(kinetic_matrix(count_z))))
    wy = jnp.asarray(split_const(left_block(kinetic_matrix(count_y))))
    order = np.arange(2 * width_x).reshape(2, grid_count, planes).transpose(1, 0, 2).reshape(-1)
    wx = jnp.asarray(split_const(left_block(kinetic_matrix(width_x))[order][:, order]))
    if (
        grid_count == 4
        and orb_count == 4
        and layers >= 4
        and planes % 8 == 0
        and count_y % (8 * LANE_ROWS) == 0
        and count_z % 128 == 0
    ):
        evolved, angle = evolve(orbitals, v_local, occupations, wz, wy)
        return turn(evolved, angle)

    weights = lax.dynamic_slice_in_dim(occupations, lax.axis_index("orb") * layers, layers, 0)

    exchange = partial(lax.all_to_all, axis_name="grid", split_axis=0, concat_axis=0, tiled=True)

    received = [
        exchange(kinetic_local(orbitals, layer, grid_count, wz, wy)) for layer in range(layers)
    ]
    density = None
    returned = []
    for layer in range(layers):
        moved, density = kinetic_across(
            received[layer], weights[layer : layer + 1], density, wx
        )
        returned.append(exchange(moved))
    share = lax.psum_scatter(density, "orb", scatter_dimension=1, tiled=True)
    share, returned[0] = lax.optimization_barrier((share, returned[0]))
    hartree_lines = poisson_shared(share)
    rows_back = lax.all_to_all(hartree_lines, "grid", split_axis=0, concat_axis=1, tiled=True)
    gathered = lax.all_gather(rows_back, "orb", axis=0, tiled=False)
    hartree = gathered.reshape(orb_count, planes, grid_count, share_y, count_z)
    hartree = hartree.transpose(1, 2, 0, 3, 4).reshape(planes, count_y, count_z)
    angle = TIME_STEP * (v_local + hartree)
    return rotate(returned, jnp.cos(angle), jnp.sin(angle))


def solution(mesh):
    return jax.shard_map(
        body,
        mesh=mesh,
        in_specs=(
            P(("groups", "orb"), None, "grid", None, None),
            P(("groups", "grid"), None, None),
            P("groups"),
        ),
        out_specs=P(("groups", "orb"), None, "grid", None, None),
        check_vma=False,
    )
```

```python
from functools import partial
import math

import jax
import jax.numpy as jnp
import ml_dtypes
import numpy as np
from jax import lax
from jax.experimental import pallas as pl
from jax.experimental.pallas import tpu as pltpu
from jax.sharding import PartitionSpec as P

TIME_STEP = 0.05
KINETIC_RATE = 0.1
HARTREE_SCALE = math.pi
HIGHEST = lax.Precision.HIGHEST
VMEM_LIMIT = 50 * 1024 * 1024


def wave_squared(length):
    ids = np.arange(length)
    signed = np.where(ids < (length + 1) // 2, ids, ids - length)
    return (2.0 * np.pi * signed / length) ** 2


def fourier(length, sign):
    ids = np.arange(length)
    return np.exp(sign * 2j * np.pi * ((ids[:, None] * ids[None, :]) % length) / length)


def kinetic_matrix(length):
    phase = np.exp(-1j * KINETIC_RATE * wave_squared(length))
    return (fourier(length, 1) / length * phase[None, :]) @ fourier(length, -1)


def left_block(matrix):
    return np.block([[matrix.real, -matrix.imag], [matrix.imag, matrix.real]])


def right_block(matrix):
    return np.block([[matrix.real, matrix.imag], [-matrix.imag, matrix.real]])


def split_const(table):
    table = np.asarray(table, np.float32)
    high = table.astype(ml_dtypes.bfloat16)
    low = (table - high.astype(np.float32)).astype(ml_dtypes.bfloat16)
    return np.stack([high, low])


def split(values):
    high = values.astype(jnp.bfloat16)
    low = (values - high.astype(jnp.float32)).astype(jnp.bfloat16)
    return high, low


def dot(left, right):
    return jnp.dot(left, right, preferred_element_type=jnp.float32)


def data_by_table(values, table):
    high, low = split(values)
    return dot(high, table[0]) + dot(high, table[1]) + dot(low, table[0])


def table_by_data(table, values):
    high, low = split(values)
    return dot(table[0], high) + dot(table[1], high) + dot(table[0], low)


def local_kernel(psi_ref, wz_ref, wy_ref, out_ref):
    _, _, bx, ny, nz = psi_ref.shape
    grid_count, _, _, vy, _ = out_ref.shape
    real_part = psi_ref[0, 0].reshape(bx * ny, nz)
    imag_part = psi_ref[0, 1].reshape(bx * ny, nz)
    turned = data_by_table(jnp.concatenate([real_part, imag_part], 1), wz_ref)
    columns = [
        jnp.concatenate(
            [turned[p * ny : (p + 1) * ny, :nz], turned[p * ny : (p + 1) * ny, nz:]], 0
        )
        for p in range(bx)
    ]
    rows = table_by_data(wy_ref, jnp.concatenate(columns, 1))
    for g in range(grid_count):
        for c in range(2):
            start = c * ny + g * vy
            for p in range(bx):
                out_ref[g, c, p] = rows[start : start + vy, p * nz : (p + 1) * nz]


def kinetic_local(orbitals, layer, grid_count, wz, wy):
    _, _, planes, ny, nz = orbitals.shape
    bx = min(4, planes)
    vy = ny // grid_count
    return pl.pallas_call(
        local_kernel,
        grid=(planes // bx,),
        in_specs=[
            pl.BlockSpec((1, 2, bx, ny, nz), lambda i: (layer, 0, i, 0, 0)),
            pl.BlockSpec(wz.shape, lambda i: (0, 0, 0)),
            pl.BlockSpec(wy.shape, lambda i: (0, 0, 0)),
        ],
        out_specs=pl.BlockSpec((grid_count, 2, bx, vy, nz), lambda i: (0, 0, i, 0, 0)),
        out_shape=jax.ShapeDtypeStruct((grid_count, 2, planes, vy, nz), jnp.float32),
        compiler_params=pltpu.CompilerParams(vmem_limit_bytes=VMEM_LIMIT),
        cost_estimate=pl.CostEstimate(
            flops=3 * 8 * planes * ny * nz * (ny + nz),
            bytes_accessed=16 * planes * ny * nz,
            transcendentals=0,
        ),
    )(orbitals, wz, wy)


def across_kernel(planes, first, weight_ref, psi_ref, wx_ref, *refs):
    if first:
        out_ref, density_ref = refs
    else:
        earlier_ref, out_ref, density_ref = refs
    depth, by, nz = psi_ref.shape
    columns = jnp.concatenate([psi_ref[:, j, :] for j in range(by)], 1)
    moved = table_by_data(wx_ref, columns)
    squares = moved * moved
    weight = weight_ref[0]
    for j in range(by):
        out_ref[:, j, :] = moved[:, j * nz : (j + 1) * nz]
    for h in range(depth // (2 * planes)):
        low = 2 * h * planes
        term = weight * (squares[low : low + planes] + squares[low + planes : low + 2 * planes])
        for j in range(by):
            value = term[:, j * nz : (j + 1) * nz]
            if not first:
                value = value + earlier_ref[h * planes : (h + 1) * planes, j, :]
            density_ref[h * planes : (h + 1) * planes, j, :] = value


def kinetic_across(received, weight, density, wx):
    grid_count, _, planes, vy, nz = received.shape
    depth = grid_count * 2 * planes
    by = min(8, vy)
    first = density is None
    block = pl.BlockSpec((depth, by, nz), lambda i: (0, i, 0))
    density_block = pl.BlockSpec((depth // 2, by, nz), lambda i: (0, i, 0))
    in_specs = [
        pl.BlockSpec(memory_space=pltpu.SMEM),
        block,
        pl.BlockSpec(wx.shape, lambda i: (0, 0, 0)),
    ]
    operands = [weight, received.reshape(depth, vy, nz), wx]
    if not first:
        in_specs.append(density_block)
        operands.append(density)
    moved, density = pl.pallas_call(
        partial(across_kernel, planes, first),
        grid=(vy // by,),
        in_specs=in_specs,
        out_specs=[block, density_block],
        out_shape=[
            jax.ShapeDtypeStruct((depth, vy, nz), jnp.float32),
            jax.ShapeDtypeStruct((depth // 2, vy, nz), jnp.float32),
        ],
        compiler_params=pltpu.CompilerParams(vmem_limit_bytes=VMEM_LIMIT),
        cost_estimate=pl.CostEstimate(
            flops=3 * 2 * depth * depth * vy * nz,
            bytes_accessed=12 * depth * vy * nz,
            transcendentals=0,
        ),
    )(*operands)
    return moved.reshape(grid_count, 2, planes, vy, nz), density


LANE_ROWS = 8
MESH = pl.DeviceIdType.MESH
EPS = float(np.finfo(np.float32).eps)


def far_factors(block):
    block = block.astype(np.clongdouble)
    norm2 = np.sum(np.abs(block) ** 2)
    residual = block.copy()
    rank = 0
    basis = []
    for _ in range(block.shape[1]):
        sizes = np.sum(np.abs(residual) ** 2, axis=1)
        if np.sum(sizes) <= (EPS * EPS) * 1e-3 * norm2:
            break
        row = residual[int(np.argmax(sizes))].conj()
        for other in basis:
            row = row - other * np.sum(other.conj() * row)
        row = row / np.sqrt(np.sum(np.abs(row) ** 2))
        basis.append(row)
        residual = residual - np.sum(residual * row[None, :], axis=1)[:, None] * row.conj()[None, :]
    gram = np.matmul(block.conj().T, block)
    for _ in range(8):
        basis = [np.sum(gram * vector[None, :], axis=1) for vector in basis]
        clean = []
        for row in basis:
            for _ in range(2):
                for other in clean:
                    row = row - other * np.sum(other.conj() * row)
            clean.append(row / np.sqrt(np.sum(np.abs(row) ** 2)))
        basis = clean
    for rank in range(1, len(basis) + 1):
        right = np.stack(basis[:rank], 1)
        left = np.matmul(block, right)
        rest = block - np.matmul(left, right.conj().T)
        if np.linalg.norm(rest.astype(np.complex128), 2) <= EPS:
            break
    return left.astype(np.complex128), right.astype(np.complex128)


def real_form(matrix):
    return np.block([[matrix.real, -matrix.imag], [matrix.imag, matrix.real]])


def stacked_table(table):
    high, low = split_const(table).astype(np.float32)
    return np.block([[high, high], [low, np.zeros_like(low)]]).astype(ml_dtypes.bfloat16)


def evolve_tables(width_x, planes):
    matrix = kinetic_matrix(width_x)
    half = 2 * planes
    left, right = far_factors(matrix[half:, :half])
    rank = -(-left.shape[1] // 2) * 2
    pad = rank - left.shape[1]
    left = np.pad(left, ((0, 0), (0, pad)))
    right = np.pad(right, ((0, 0), (0, pad)))
    near = matrix[:planes, :planes]
    sides = []
    for core in range(2):
        mine = slice(core * planes, (core + 1) * planes)
        theirs = slice((1 - core) * planes, (2 - core) * planes)
        sides.append(
            (left[mine], right[mine], far_factors(matrix[theirs, mine]), far_factors(matrix[mine, theirs]))
        )
    core_rank = max(s[2][0].shape[1] for s in sides)
    core_rank = -(-core_rank // 4) * 4
    widen = lambda m: np.pad(m, ((0, 0), (0, core_rank - m.shape[1])))
    far = -(-2 * rank // 8) * 8
    gather, spread = [], []
    for mine_left, mine_right, (_, give), (take, _) in sides:
        rows = real_form(mine_right.conj().T)
        rows = np.concatenate([rows, np.zeros((far - rows.shape[0], rows.shape[1]))], 0)
        core_rows = real_form(widen(give).conj().T)
        gather.append(stacked_table(np.concatenate([rows, core_rows], 0)))
        far_columns = real_form(mine_left)
        far_columns = np.pad(far_columns, ((0, 0), (0, far - far_columns.shape[1])))
        spread.append(
            stacked_table(np.concatenate([real_form(near), real_form(widen(take)), far_columns], 1))
        )
    return np.stack(gather), np.stack(spread), 2 * rank, far, 2 * core_rank


def stack_split(values):
    high, low = split(values)
    return jnp.concatenate([high, low], 0)


def split_three(values):
    high = values.astype(jnp.bfloat16)
    rest = values - high.astype(jnp.float32)
    middle = rest.astype(jnp.bfloat16)
    low = (rest - middle.astype(jnp.float32)).astype(jnp.bfloat16)
    return [high, middle, low]


def six_table(table):
    parts, rest = [], np.asarray(table, np.float32)
    for _ in range(3):
        parts.append(rest.astype(ml_dtypes.bfloat16).astype(np.float32))
        rest = rest - parts[-1]
    high, middle, low = parts
    return np.concatenate([high, high, high, middle, middle, low], 1).astype(ml_dtypes.bfloat16)


def six_parts(values):
    high, middle, low = split_three(values)
    return [high, middle, low, high, middle, high]


def exact_left(table_ref, values):
    return dot(table_ref[...], jnp.concatenate(six_parts(values), 0))


def exact_right(values, table_ref):
    parts = six_parts(values)
    width = values.shape[1]
    total = None
    for pair in range(3):
        data = jnp.concatenate(parts[2 * pair : 2 * pair + 2], 1)
        term = dot(data, table_ref[2 * pair * width : 2 * (pair + 1) * width, :])
        total = term if total is None else total + term
    return total


def real_basis(length):
    ids = np.arange(length)
    angle = 2.0 * np.pi * ((ids[:, None] * ids[None, :]) % length) / length
    table = np.where(ids[None, :] <= length // 2, np.cos(angle), np.sin(angle))
    single = (ids == 0) | (2 * ids == length)
    return table * np.where(single, 1.0, math.sqrt(2.0))[None, :] / math.sqrt(length)


def rows_at(ref, row):
    return ref[pl.ds(row, ref.shape[0] // LANE_ROWS, stride=LANE_ROWS), :]


def put_rows(ref, row, values):
    ref[pl.ds(row, ref.shape[0] // LANE_ROWS, stride=LANE_ROWS), :] = values


def tile_of(index):
    return pl.ds(pl.multiple_of(index * LANE_ROWS, LANE_ROWS), LANE_ROWS)


def evolve_kernel(
    layers, far_rows, far, near_rows, lag,
    weight_ref, wave_ref, psi_ref, local_ref, wz_ref, wy_ref, gather_ref, spread_ref,
    qz_ref, qzt_ref, qy_ref, qyt_ref, qx_ref, qxt_ref, plane_wave_ref,
    out_ref, angle_ref,
    stage, phi, give_far, give_near, got_far, got_near, far_field, result, density,
    outer_sum, middle_sum, total, spectrum, lines, returned, local,
    in_sem, out_sem, p_send, p_recv, q_send, q_recv, y_send, y_recv, f_send, f_recv,
    a_send, a_recv, m_send, m_recv, t_send, t_recv, l_send, l_recv, b_send, b_recv, d_send, d_recv, v_sem,
):
    _, _, planes, ny, nz = psi_ref.shape
    groups = ny // LANE_ROWS
    tiles = groups // 2
    units = layers * tiles
    bx = stage.shape[2]
    per_layer = planes // bx
    steps = layers * per_layer
    paired = (layers - 3) * tiles
    place = lax.axis_index("grid")
    core = lax.rem(place, 2)
    sibling = place + 1 - 2 * core
    across = lax.rem(place + 2, 4)
    depth = lax.axis_index("orb")
    outer = (depth == 0) | (depth == 3)
    inner = (depth == 1) | (depth == 2)
    toward = 1 + depth // 3
    outward = jnp.where(depth == 1, 0, 3)
    middle = jnp.where(depth == 1, 2, 1)

    def where_is(unit):
        late = unit - paired
        layer = jnp.where(late < 0, unit // tiles, layers - 3 + lax.rem(jnp.maximum(late, 0), 3))
        tile = jnp.where(late < 0, lax.rem(unit, tiles), jnp.maximum(late, 0) // 3)
        return layer, tile

    def remote(source, target, send_sem, recv_sem, device):
        return pltpu.make_async_remote_copy(
            src_ref=source, dst_ref=target, send_sem=send_sem, recv_sem=recv_sem,
            device_id=device, device_id_type=MESH,
        )

    def far_copy(unit):
        return remote(
            give_far.at[lax.rem(unit, 4), 1 - core], got_far.at[unit],
            p_send.at[unit], p_recv.at[unit], {"grid": sibling},
        )

    def near_copy(unit):
        return remote(
            give_near.at[lax.rem(unit, 4)], got_near.at[unit],
            q_send.at[unit], q_recv.at[unit], {"grid": sibling},
        )

    def across_copy(unit):
        return remote(
            got_far.at[unit], far_field.at[unit, core, pl.ds(0, far_rows * LANE_ROWS)],
            y_send.at[unit], y_recv.at[unit], {"grid": across},
        )

    def share_copy(unit):
        held = far_field.at[unit, core, pl.ds(0, far_rows * LANE_ROWS)]
        return remote(held, held, f_send.at[unit], f_recv.at[unit], {"grid": sibling})

    piece = planes * LANE_ROWS // 2

    def piece_of(ref, g, p):
        return ref.at[g, pl.ds(p * piece, piece)]

    def outer_copy(g, p):
        return remote(
            piece_of(density, g, p), piece_of(outer_sum, g, p), a_send.at[g, p], a_recv.at[g, p], {"orb": toward}
        )

    def middle_copy(g, p):
        return remote(
            piece_of(density, g, p), piece_of(middle_sum, g, p), m_send.at[g, p], m_recv.at[g, p], {"orb": middle}
        )

    def total_copy(g, p):
        held = piece_of(total, g, p)
        return remote(held, held, t_send.at[g, p], t_recv.at[g, p], {"orb": outward})

    def pieces(tile):
        return [(2 * tile + g, p) for g in range(2) for p in range(2)]

    def load_copy(step):
        layer, part = step // per_layer, lax.rem(step, per_layer)
        slot = lax.rem(step, 3)
        return pltpu.make_async_copy(
            psi_ref.at[layer, :, pl.ds(part * bx, bx)], stage.at[slot], in_sem.at[slot]
        )

    def result_copy(unit, half):
        layer, tile = where_is(unit)
        slot = lax.rem(unit, 3)
        return pltpu.make_async_copy(
            result.at[slot, half],
            out_ref.at[layer, 2 * tile + half],
            out_sem.at[slot, half],
        )

    load_copy(0).start()
    load_copy(1).start()
    local_copy = pltpu.make_async_copy(local_ref, local, v_sem)
    local_copy.start()
    if far > far_rows:
        far_field[:, :, far_rows * LANE_ROWS :] = jnp.zeros((units, 2, (far - far_rows) * LANE_ROWS, nz), jnp.float32)
    density[...] = jnp.zeros_like(density)
    barrier = pltpu.get_barrier_semaphore()
    for k in range(1, 4):
        pl.semaphore_signal(barrier, inc=1, device_id={"grid": lax.rem(place + k, 4)}, device_id_type=MESH)

    @pl.when(outer)
    def _():
        pl.semaphore_signal(barrier, inc=1, device_id={"orb": toward}, device_id_type=MESH)

    @pl.when(inner)
    def _():
        pl.semaphore_signal(barrier, inc=1, device_id={"orb": outward}, device_id_type=MESH)
        pl.semaphore_signal(barrier, inc=1, device_id={"orb": middle}, device_id_type=MESH)

    def plane_step(step, carry):
        @pl.when(step + 2 < steps)
        def _():
            load_copy(step + 2).start()

        load_copy(step).wait()
        layer, part = step // per_layer, lax.rem(step, per_layer)
        slot = lax.rem(step, 3)
        real_part = stage[slot, 0].reshape(bx * ny, nz)
        imag_part = stage[slot, 1].reshape(bx * ny, nz)
        turned = data_by_table(jnp.concatenate([real_part, imag_part], 1), wz_ref)
        columns = [
            jnp.concatenate([turned[p * ny : (p + 1) * ny, :nz], turned[p * ny : (p + 1) * ny, nz:]], 0)
            for p in range(bx)
        ]
        rows = table_by_data(wy_ref, jnp.concatenate(columns, 1))
        for c in range(2):
            for p in range(bx):
                block = rows[c * ny : (c + 1) * ny, p * nz : (p + 1) * nz]
                phi[layer, :, tile_of(c * planes + part * bx + p), :] = block.reshape(groups, LANE_ROWS, nz)
        return carry

    def gather_step(unit):
        layer, tile = where_is(unit)
        slot = lax.rem(unit, 4)

        @pl.when(unit >= 4)
        def _():
            far_copy(unit - 4).wait_send()
            near_copy(unit - 4).wait_send()

        for half in range(2):
            for part in range(2):
                ids = range(4 * part, 4 * part + 4)
                source = phi.at[layer, 2 * tile + half]
                data = jnp.concatenate([rows_at(source, i) for i in ids], 1)
                both = dot(gather_ref[core], stack_split(data))
                joined = both[: far + near_rows] + both[far + near_rows :]
                for k, i in enumerate(ids):
                    block = joined[:, k * nz : (k + 1) * nz]
                    put_rows(give_far.at[slot, half], i, block[:far_rows])
                    put_rows(give_near.at[slot, half], i, block[far:])

    def sum_step(unit):
        far_copy(unit).wait_recv()
        got_far[unit] = got_far[unit] + give_far[lax.rem(unit, 4), core]

    def spread_step(unit):
        layer, tile = where_is(unit)
        slot = lax.rem(unit, 3)
        near_copy(unit).wait_recv()
        share_copy(unit).wait_recv()

        @pl.when(unit >= 3)
        def _():
            result_copy(unit - 3, 0).wait()
            result_copy(unit - 3, 1).wait()

        weight = weight_ref[depth * layers + layer]
        for half in range(2):
            for part in range(2):
                ids = range(4 * part, 4 * part + 4)
                data = jnp.concatenate(
                    [
                        jnp.concatenate(
                            [
                                rows_at(phi.at[layer, 2 * tile + half], i),
                                rows_at(got_near.at[unit, half], i),
                                rows_at(far_field.at[unit, half], i),
                            ],
                            0,
                        )
                        for i in ids
                    ],
                    1,
                )
                both = dot(spread_ref[core], stack_split(data))
                moved = both[: 2 * planes] + both[2 * planes :]
                squares = moved * moved
                term = weight * (squares[:planes] + squares[planes:])
                for k, i in enumerate(ids):
                    put_rows(result.at[slot, half], i, moved[:, k * nz : (k + 1) * nz])
                    summed = density.at[2 * tile + half]
                    put_rows(summed, i, rows_at(summed, i) + term[:, k * nz : (k + 1) * nz])

    def send(unit):
        far_copy(unit).start()
        near_copy(unit).start()

    def forward(unit):
        across_copy(unit).wait_recv()
        share_copy(unit).start()

    def write(unit):
        result_copy(unit, 0).start()
        result_copy(unit, 1).start()

    def start_outer(tile):
        for g, p in pieces(tile):
            outer_copy(g, p).start()

    def add_outer(tile):
        held = None
        for g, p in pieces(tile):
            outer_copy(g, p).wait_recv()
            rows = pl.ds(p * piece, piece)
            density[g, rows] = density[g, rows] + outer_sum[g, rows]
            if held is not None:
                middle_copy(*held).start()
            held = (g, p)

    def start_middle(tile):
        middle_copy(2 * tile + 1, 1).start()

    def add_middle(tile):
        held = None
        for g, p in pieces(tile):
            middle_copy(g, p).wait_recv()
            rows = pl.ds(p * piece, piece)
            total[g, rows] = density[g, rows] + middle_sum[g, rows]
            if held is not None:
                total_copy(*held).start()
            held = (g, p)

    def start_total(tile):
        total_copy(2 * tile + 1, 1).start()
        for g in range(2):
            flatten(2 * tile + g)

    def flatten(g):
        outer_sum[g] = exact_right(total[g], qz_ref)

    def receive(tile):
        for g in range(2):
            for p in range(2):
                total_copy(2 * tile + g, p).wait_recv()
            flatten(2 * tile + g)

    def prepared(t):
        late = jnp.maximum(t - 2, 0)
        return jnp.minimum(per_layer + (late * (layers - 1) * per_layer) // (paired - 2), steps)

    first_forward = 3 + lag
    first_spread = first_forward + 2
    ready = first_spread + 1
    last = ready + 15

    def tick(t, carry):
        def stage_at(start, action):
            unit = t - start

            @pl.when((unit >= 0) & (unit < units))
            def _():
                action(unit)

        def reduce_at(start, who, action):
            late = t - start - paired

            @pl.when((late >= 0) & (late < 3 * tiles) & (lax.rem(late + 3 * units, 3) == 2) & who)
            def _():
                action(late // 3)

        stage_at(1, send)
        stage_at(3, lambda unit: across_copy(unit).start())
        stage_at(ready, write)
        reduce_at(ready, outer, start_outer)
        reduce_at(ready + 4, inner, add_outer)
        reduce_at(ready + 5, inner, start_middle)
        reduce_at(ready + 9, inner, add_middle)
        reduce_at(ready + 10, inner, start_total)
        reduce_at(ready + 15, outer, receive)
        lax.fori_loop(prepared(t), prepared(t + 1), plane_step, 0)
        stage_at(2, sum_step)
        stage_at(0, gather_step)
        stage_at(first_forward, forward)
        stage_at(first_spread, spread_step)
        return carry

    lax.fori_loop(0, per_layer, plane_step, 0)

    @pl.when(outer)
    def _():
        pl.semaphore_wait(barrier, 4)

    @pl.when(inner)
    def _():
        pl.semaphore_wait(barrier, 5)

    lax.fori_loop(0, last + units, tick, 0)

    local_copy.wait()

    four = 4

    def spectrum_step(part, carry):
        ids = [part * four + p for p in range(four)]
        moved = exact_left(
            qyt_ref, jnp.concatenate([outer_sum[:, tile_of(x), :].reshape(ny, nz) for x in ids], 1)
        )
        for p, x in enumerate(ids):
            spectrum[:, tile_of(x), :] = moved[:, p * nz : (p + 1) * nz].reshape(groups, LANE_ROWS, nz)
        return carry

    lax.fori_loop(0, planes // four, spectrum_step, 0)
    share = groups // 8
    span = planes * LANE_ROWS
    mine = lax.rem(depth, 2) * (groups // 2)
    other = groups // 2 - mine
    partner = depth + 1 - 2 * lax.rem(depth, 2)

    def lines_of(device):
        return pl.ds(pl.multiple_of(device * span, span), span)

    def line_copy(g, k):
        peer = lax.rem(place + k, 4)
        return remote(
            spectrum.at[mine + peer * share + g], lines.at[g, lines_of(place)],
            l_send.at[g, k - 1], l_recv.at[g, k - 1], {"grid": peer},
        )

    def back_copy(g, k):
        peer = lax.rem(place + k, 4)
        return remote(
            lines.at[g, lines_of(peer)], returned.at[mine + place * share + g],
            b_send.at[g, k - 1], b_recv.at[g, k - 1], {"grid": peer},
        )

    def pair_copy(row):
        return remote(
            returned.at[row], returned.at[row],
            d_send.at[row], d_recv.at[row], {"orb": partner},
        )

    for g in range(share):
        for k in (2, 3, 1):
            line_copy(g, k).start()
        lines[g, lines_of(place)] = spectrum[mine + place * share + g]

    for g in range(share):
        for k in (1, 2, 3):
            line_copy(g, k).wait_recv()
        for part in range(2):
            ids = range(4 * part, 4 * part + 4)
            data = jnp.concatenate([rows_at(lines.at[g], i) for i in ids], 1)
            modes = exact_left(qxt_ref, data)
            scaled = []
            for k, i in enumerate(ids):
                waves = plane_wave_ref[...] + wave_ref[(mine + place * share + g) * LANE_ROWS + i]
                anchor = waves <= 0.0
                kernel = jnp.where(anchor, 0.0, HARTREE_SCALE / jnp.where(anchor, 1.0, waves))
                scaled.append(modes[:, k * nz : (k + 1) * nz] * kernel)
            moved = exact_left(qx_ref, jnp.concatenate(scaled, 1))
            for k, i in enumerate(ids):
                put_rows(lines.at[g], i, moved[:, k * nz : (k + 1) * nz])
        row = mine + place * share + g
        returned[row] = lines[g, lines_of(place)]
        for k in (2, 1, 3):
            back_copy(g, k).start()
        pair_copy(row).start()
    for g in range(share):
        for k in (1, 2, 3):
            line_copy(g, k).wait_send()

    def straighten(row):
        spectrum[row] = exact_right(returned[row], qzt_ref)

    for g in range(share):
        straighten(mine + place * share + g)
    for g in range(share):
        for k in (3, 1, 2):
            row = mine + lax.rem(place + 4 - k, 4) * share + g
            back_copy(g, k).wait_recv()
            pair_copy(row).start()
            straighten(row)

    def finish(unit, carry):
        across_copy(unit).wait_send()
        share_copy(unit).wait_send()

        @pl.when(unit >= units - 4)
        def _():
            far_copy(unit).wait_send()
            near_copy(unit).wait_send()

        @pl.when(unit >= units - 3)
        def _():
            result_copy(unit, 0).wait()
            result_copy(unit, 1).wait()

        return carry

    lax.fori_loop(0, units, finish, 0)

    @pl.when(outer)
    def _():
        for g in range(groups):
            for p in range(2):
                outer_copy(g, p).wait_send()

    @pl.when(inner)
    def _():
        for g in range(groups):
            for p in range(2):
                middle_copy(g, p).wait_send()
                total_copy(g, p).wait_send()

    for k in (0, 3, 1, 2):
        for g in range(share):
            row = other + lax.rem(place + 4 - k, 4) * share + g
            pair_copy(row).wait_recv()
            straighten(row)

    def potential_step(part, carry):
        ids = [part * four + p for p in range(four)]
        moved = exact_left(
            qy_ref, jnp.concatenate([spectrum[:, tile_of(x), :].reshape(ny, nz) for x in ids], 1)
        )
        for p, x in enumerate(ids):
            angle_ref[x] = TIME_STEP * (local[x] + moved[:, p * nz : (p + 1) * nz])
        return carry

    lax.fori_loop(0, planes // four, potential_step, 0)
    for g in range(share):
        for k in (1, 2, 3):
            back_copy(g, k).wait_send()

    def settle(row, carry):
        pair_copy(mine + row).wait_send()
        return carry

    lax.fori_loop(0, groups // 2, settle, 0)


def evolve(orbitals, v_local, occupations, wz, wy):
    layers, _, planes, ny, nz = orbitals.shape
    width_x = 4 * planes
    gather, spread, far_rows, far, near_rows = evolve_tables(width_x, planes)
    groups = ny // LANE_ROWS
    tiles = groups // 2
    units = layers * tiles
    f32 = jnp.float32
    squares = [wave_squared(n).astype(np.float32) for n in (width_x, ny, nz)]
    plane_wave = squares[0][:, None] + squares[2][None, :]
    basis = [real_basis(n) for n in (width_x, ny, nz)]
    tables = [
        six_table(basis[2].T).T, six_table(basis[2]).T, six_table(basis[1]), six_table(basis[1].T),
        six_table(basis[0]), six_table(basis[0].T), plane_wave,
    ]
    vmem = pl.BlockSpec(memory_space=pltpu.VMEM)
    smem = pl.BlockSpec(memory_space=pltpu.SMEM)
    anywhere = pl.BlockSpec(memory_space=pl.ANY)
    dma = pltpu.SemaphoreType.DMA
    field = pltpu.VMEM((groups, planes * LANE_ROWS, nz), f32)
    evolved, angle = pl.pallas_call(
        partial(evolve_kernel, layers, far_rows, far, near_rows, 3),
        in_specs=[smem, smem, anywhere, anywhere] + [vmem] * 11,
        out_specs=[anywhere, vmem],
        out_shape=[
            jax.ShapeDtypeStruct((layers, groups, 2 * planes * LANE_ROWS, nz), f32),
            jax.ShapeDtypeStruct((planes, ny, nz), f32),
        ],
        scratch_shapes=[
            pltpu.VMEM((3, 2, 8, ny, nz), f32),
            pltpu.VMEM((layers, groups, 2 * planes * LANE_ROWS, nz), f32),
            pltpu.VMEM((4, 2, far_rows * LANE_ROWS, nz), f32),
            pltpu.VMEM((4, 2, near_rows * LANE_ROWS, nz), f32),
            pltpu.VMEM((units, far_rows * LANE_ROWS, nz), f32),
            pltpu.VMEM((units, 2, near_rows * LANE_ROWS, nz), f32),
            pltpu.VMEM((units, 2, far * LANE_ROWS, nz), f32),
            pltpu.VMEM((3, 2, 2 * planes * LANE_ROWS, nz), f32),
            field, field, field, field, field,
            pltpu.VMEM((groups // 8, width_x * LANE_ROWS, nz), f32),
            field,
            pltpu.VMEM((planes, ny, nz), f32),
            dma((3,)),
            dma((3, 2)),
        ]
        + [dma((units,))] * 8
        + [dma((groups, 2))] * 6
        + [dma((groups // 8, 3))] * 4
        + [dma((groups,))] * 2
        + [pltpu.SemaphoreType.DMA],
        compiler_params=pltpu.CompilerParams(
            vmem_limit_bytes=63 * 1024 * 1024, collective_id=0, has_side_effects=True
        ),
        cost_estimate=pl.CostEstimate(
            flops=40 * layers * planes * ny * nz * (ny + nz), bytes_accessed=16 * layers * planes * ny * nz, transcendentals=0
        ),
    )(occupations, jnp.asarray(squares[1]), orbitals, v_local, wz, wy, *map(jnp.asarray, [gather, spread] + tables))
    return evolved.reshape(layers, groups, 2, planes, LANE_ROWS, nz), angle


def cos_sin(angle):
    turns = jnp.floor(angle * (2.0 / math.pi) + 0.5)
    rest = ((angle - turns * 1.5703125) - turns * 4.837512969970703125e-4) - turns * 7.549789954891882e-8
    square = rest * rest
    sine = ((-1.9515295891e-4 * square + 8.3321608736e-3) * square - 1.6666654611e-1) * square * rest + rest
    cosine = (
        (2.443315711809948e-5 * square - 1.388731625493765e-3) * square + 4.166664568298827e-2
    ) * square * square - 0.5 * square + 1.0
    quarter = turns.astype(jnp.int32) & 3
    odd = (quarter & 1) == 1
    first = jnp.where(odd, sine, cosine)
    second = jnp.where(odd, cosine, sine)
    first = jnp.where((quarter == 1) | (quarter == 2), -first, first)
    second = jnp.where(quarter >= 2, -second, second)
    return first, second


def turn_kernel(psi_ref, angle_ref, out_ref):
    cosine, sine = cos_sin(angle_ref[...])
    for g in range(psi_ref.shape[1]):
        band = slice(g * LANE_ROWS, (g + 1) * LANE_ROWS)
        turn_re, turn_im = cosine[:, band], sine[:, band]
        for l in range(psi_ref.shape[0]):
            real_part, imag_part = psi_ref[l, g, 0], psi_ref[l, g, 1]
            out_ref[l, 0, :, band, :] = real_part * turn_re + imag_part * turn_im
            out_ref[l, 1, :, band, :] = imag_part * turn_re - real_part * turn_im


def turn(evolved, angle):
    layers, groups, _, planes, _, nz = evolved.shape
    ny = groups * LANE_ROWS
    bx = min(16, planes)
    field_block = pl.BlockSpec((bx, ny, nz), lambda i: (i, 0, 0))
    return pl.pallas_call(
        turn_kernel,
        grid=(planes // bx,),
        in_specs=[
            pl.BlockSpec((layers, groups, 2, bx, LANE_ROWS, nz), lambda i: (0, 0, 0, i, 0, 0)),
            field_block,
        ],
        out_specs=pl.BlockSpec((layers, 2, bx, ny, nz), lambda i: (0, 0, i, 0, 0)),
        out_shape=jax.ShapeDtypeStruct((layers, 2, planes, ny, nz), jnp.float32),
        compiler_params=pltpu.CompilerParams(vmem_limit_bytes=63 * 1024 * 1024),
    )(evolved, angle)


def rotate_kernel(layers, *refs):
    cos_ref, sin_ref = refs[layers], refs[layers + 1]
    out_ref = refs[layers + 2]
    grid_count, _, _, vy, _ = refs[0].shape
    for g in range(grid_count):
        band = slice(g * vy, (g + 1) * vy)
        cosine = cos_ref[:, band, :]
        sine = sin_ref[:, band, :]
        for l in range(layers):
            real_part = refs[l][g, 0]
            imag_part = refs[l][g, 1]
            out_ref[l, 0, :, band, :] = real_part * cosine + imag_part * sine
            out_ref[l, 1, :, band, :] = imag_part * cosine - real_part * sine


def rotate(returned, cosine, sine):
    layers = len(returned)
    grid_count, _, planes, vy, nz = returned[0].shape
    ny = grid_count * vy
    bx = min(4, planes)
    field_block = pl.BlockSpec((bx, ny, nz), lambda i: (i, 0, 0))
    return pl.pallas_call(
        partial(rotate_kernel, layers),
        grid=(planes // bx,),
        in_specs=[pl.BlockSpec((grid_count, 2, bx, vy, nz), lambda i: (0, 0, i, 0, 0))] * layers
        + [field_block, field_block],
        out_specs=pl.BlockSpec((layers, 2, bx, ny, nz), lambda i: (0, 0, i, 0, 0)),
        out_shape=jax.ShapeDtypeStruct((layers, 2, planes, ny, nz), jnp.float32),
        compiler_params=pltpu.CompilerParams(vmem_limit_bytes=VMEM_LIMIT),
    )(*returned, cosine, sine)


def table_of(matrix):
    return (np.asarray(matrix.real, np.float32), np.asarray(matrix.imag, np.float32))


def apply_along(values, table, axis):
    contracted = jnp.tensordot(values, table, axes=([axis], [0]), precision=HIGHEST)
    return jnp.moveaxis(contracted, -1, axis)


def complex_along(real_part, imag_part, matrix, axis):
    table_re, table_im = table_of(matrix)
    new_re = apply_along(real_part, table_re, axis) - apply_along(imag_part, table_im, axis)
    new_im = apply_along(real_part, table_im, axis) + apply_along(imag_part, table_re, axis)
    return (new_re, new_im)


def coulomb_kernel(squares_x, squares_y, squares_z):
    total = squares_x[:, None, None] + squares_y[None, :, None] + squares_z[None, None, :]
    anchor = total <= 0.0
    return jnp.where(anchor, 0.0, HARTREE_SCALE / jnp.where(anchor, 1.0, total))


def poisson_shared(density):
    width_x, _, count_z = density.shape
    span_count = lax.axis_size("grid") * lax.axis_size("orb")
    block_x = width_x // span_count
    forward_z = table_of(fourier(count_z, -1))
    real_part, imag_part = (apply_along(density, forward_z[0], 2), apply_along(density, forward_z[1], 2))
    real_part, imag_part = complex_along(real_part, imag_part, fourier(width_x, -1), 0)
    spread = lax.all_to_all(
        jnp.stack([real_part, imag_part], 0),
        ("grid", "orb"),
        split_axis=1,
        concat_axis=2,
        tiled=True,
    )
    count_y = spread.shape[2]
    real_part, imag_part = complex_along(spread[0], spread[1], fourier(count_y, -1), 1)
    start_x = lax.axis_index(("grid", "orb")) * block_x
    squares_x = lax.dynamic_slice_in_dim(
        jnp.asarray(wave_squared(width_x), jnp.float32), start_x, block_x, 0
    )
    kernel = coulomb_kernel(
        squares_x,
        np.asarray(wave_squared(count_y), np.float32),
        np.asarray(wave_squared(count_z), np.float32),
    )
    real_part, imag_part = complex_along(
        real_part * kernel, imag_part * kernel, fourier(count_y, 1) / count_y, 1
    )
    back = lax.all_to_all(
        jnp.stack([real_part, imag_part], 0),
        ("grid", "orb"),
        split_axis=2,
        concat_axis=1,
        tiled=True,
    )
    real_part, imag_part = complex_along(back[0], back[1], fourier(width_x, 1) / width_x, 0)
    inverse_z = table_of(fourier(count_z, 1) / count_z)
    return apply_along(real_part, inverse_z[0], 2) - apply_along(imag_part, inverse_z[1], 2)


def body(orbitals, v_local, occupations):
    layers, _, planes, count_y, count_z = orbitals.shape
    grid_count = lax.axis_size("grid")
    orb_count = lax.axis_size("orb")
    width_x = planes * grid_count
    share_y = count_y // (grid_count * orb_count)
    wz = jnp.asarray(split_const(right_block(kinetic_matrix(count_z))))
    wy = jnp.asarray(split_const(left_block(kinetic_matrix(count_y))))
    order = np.arange(2 * width_x).reshape(2, grid_count, planes).transpose(1, 0, 2).reshape(-1)
    wx = jnp.asarray(split_const(left_block(kinetic_matrix(width_x))[order][:, order]))
    if (
        grid_count == 4
        and orb_count == 4
        and layers >= 4
        and planes % 8 == 0
        and count_y % (8 * LANE_ROWS) == 0
        and count_z % 128 == 0
    ):
        evolved, angle = evolve(orbitals, v_local, occupations, wz, wy)
        return turn(evolved, angle)

    weights = lax.dynamic_slice_in_dim(occupations, lax.axis_index("orb") * layers, layers, 0)

    exchange = partial(lax.all_to_all, axis_name="grid", split_axis=0, concat_axis=0, tiled=True)

    received = [
        exchange(kinetic_local(orbitals, layer, grid_count, wz, wy)) for layer in range(layers)
    ]
    density = None
    returned = []
    for layer in range(layers):
        moved, density = kinetic_across(
            received[layer], weights[layer : layer + 1], density, wx
        )
        returned.append(exchange(moved))
    share = lax.psum_scatter(density, "orb", scatter_dimension=1, tiled=True)
    share, returned[0] = lax.optimization_barrier((share, returned[0]))
    hartree_lines = poisson_shared(share)
    rows_back = lax.all_to_all(hartree_lines, "grid", split_axis=0, concat_axis=1, tiled=True)
    gathered = lax.all_gather(rows_back, "orb", axis=0, tiled=False)
    hartree = gathered.reshape(orb_count, planes, grid_count, share_y, count_z)
    hartree = hartree.transpose(1, 2, 0, 3, 4).reshape(planes, count_y, count_z)
    angle = TIME_STEP * (v_local + hartree)
    return rotate(returned, jnp.cos(angle), jnp.sin(angle))


def solution(mesh):
    return jax.shard_map(
        body,
        mesh=mesh,
        in_specs=(
            P(("groups", "orb"), None, "grid", None, None),
            P(("groups", "grid"), None, None),
            P("groups"),
        ),
        out_specs=P(("groups", "orb"), None, "grid", None, None),
        check_vma=False,
    )
```
